128 devices in a mesh: task: 8 (over x, core), dp: 16 (over z, y).
Axes of the slice: x: 4, y: 4, z: 4, core: 2. Of those that a mesh axis runs over, the one named last changes fastest.
Arguments:
- inputs: bfloat16 [8, 2, 8192, 1024], P('task', None, 'dp'), may hold values from -48 to 48
- labels: int32 [8, 2, 8192], P('task', None, 'dp'), may hold values from 0 to 999
- w_hidden: float32 [8, 1024, 1024], P('task', 'dp'), may hold values from -6 to 6
- w_out: float32 [8, 1024, 1000], P('task', 'dp'), may hold values from -12 to 12
- mom_hidden: float32 [8, 1024, 1024], P('task', 'dp'), may hold values from -0.6 to 0.6
- mom_out: float32 [8, 1024, 1000], P('task', 'dp'), may hold values from -0.6 to 0.6
- signs: int32 [8], P('task'), may hold values from -1 to 1, as said below
- perturb: float32 [8, 512, 512], P('task', 'dp'), may hold values from -6 to 6
- hyper_in: float32 [8, 512], replicated, may hold values from -2 to 2
- hyper_mid: float32 [512, 512], P('dp'), may hold values from -0.25 to 0.25
- hyper_out: float32 [512, 21], replicated, may hold values from -0.25 to 0.25
Outputs:
- new_hidden: float32 [8, 1024, 1024], P('task', 'dp')
- new_out: float32 [8, 1024, 1000], P('task', 'dp')
- new_mom_hidden: float32 [8, 1024, 1024], P('task', 'dp')
- new_mom_out: float32 [8, 1024, 1000], P('task', 'dp')
- task_losses: float32 [8, 2], P('task')
- meta_grad: float32 [512, 512], P('dp')
The draws below stay inside these ranges and needn't reach their ends.
Inputs may be any that keep to these rules, and one draw needn't show every extreme that they name: `signs`: each entry is +1 or -1.
All inputs are finite; a program needn't handle non-finite values.
Results may differ from the reference program's by a relative error of at most 0.01045.
The reference program's roundings to bfloat16 on the way count: a program that leaves them out, or rounds other values in their place, can miss the bound.
Values may be sent and summed in bfloat16 or wider, within the bound.
No kernel may reach another device: no remote copies, remote signals or barrier semaphores. Data moves between devices by JAX's collectives and lax.ppermute only.
A program may use at most 128 MiB of HBM per device.

```python
import jax
import jax.numpy as jnp
from jax import lax

DIN = 1024
HID = 1024
CLASSES = 1000
HYP = 512
TFEAT = 8
STEPS = 2
NGEN = 21
BATCH = 8192
TASKS = 8


def draw_inputs(key, part):
    base_key = jax.random.fold_in(key, 0)
    values = jnp.clip(jax.random.normal(base_key, (TASKS, STEPS, BATCH, DIN), jnp.float32), -6.0, 6.0)
    return values.astype(jnp.bfloat16)


def draw_w_out(key, part):
    base_key = jax.random.fold_in(key, 0)
    values = jnp.clip(jax.random.normal(base_key, (TASKS, HID, CLASSES), jnp.float32), -6.0, 6.0)
    return values


def draw_signs(key, part):
    return (2 * jax.random.randint(key, (TASKS,), 0, 2) - 1).astype(jnp.int32)


def with_ends(entries, own_key, low, top_value):
    extent = entries.shape
    spot = [jax.random.randint(jax.random.fold_in(own_key, axis), (), 0, extent[axis]) for axis in range(len(extent))]
    entries = entries.at[tuple(spot)].set(low)
    longest = extent.index(max(extent))
    spot[longest] = (spot[longest] + 1) % extent[longest]
    return entries.at[tuple(spot)].set(top_value)


def shard_levels(stream_key, dims, pieces, least, largest):
    level, own = 1.0, jax.random.fold_in(stream_key, 6)
    for dim, shards_of in pieces:
        heights = jnp.exp(jax.random.uniform(jax.random.fold_in(own, dim), (shards_of,), jnp.float32, least / len(pieces), largest / len(pieces)))
        level = level * jnp.repeat(heights, dims[dim] // shards_of).reshape([-1 if axis == dim else 1 for axis in range(len(dims))])
    return level


def gaussian(key, extent, deviation, bound, pieces=(), kind=jnp.bfloat16):
    array = deviation * jax.random.normal(key, extent, jnp.float32)
    if pieces:
        array = array * shard_levels(key, extent, pieces, -0.22, 0.18)
    return jnp.clip(array, -bound, bound).astype(kind)


def setup_inputs(seed: int = 0) -> dict:
    keys = jax.random.split(jax.random.key(seed), 12)
    inputs = draw_inputs(jax.random.fold_in(keys[11], 71), 0)
    labels = with_ends(jax.random.randint(keys[1], (TASKS, STEPS, BATCH), 0, CLASSES), jax.random.fold_in(keys[1], 1), 0, CLASSES - 1).astype(jnp.int32)
    w_hidden = gaussian(keys[2], (TASKS, DIN, HID), 1.0, 6.0, ((0, 8), (1, 16)), jnp.float32)
    w_out = draw_w_out(jax.random.fold_in(keys[11], 71), 0)
    mom_hidden = gaussian(keys[4], (TASKS, DIN, HID), 0.1, 0.6, ((0, 8), (1, 16)), jnp.float32)
    mom_out = gaussian(keys[5], (TASKS, HID, CLASSES), 0.1, 0.6, ((0, 8), (1, 16)), jnp.float32)
    signs = draw_signs(jax.random.fold_in(keys[11], 71), 0)
    perturb = gaussian(keys[7], (TASKS, HYP, HYP), 1.0, 6.0, ((0, 8), (1, 16)), jnp.float32)
    hyper_in = gaussian(keys[8], (TFEAT, HYP), TFEAT ** -0.5, 2.0, (), jnp.float32)
    hyper_mid = gaussian(keys[9], (HYP, HYP), HYP ** -0.5, 0.25, ((0, 16),), jnp.float32)
    hyper_out = gaussian(keys[10], (HYP, NGEN), HYP ** -0.5, 0.25, (), jnp.float32)
    return dict(inputs=inputs, labels=labels, w_hidden=w_hidden, w_out=w_out, mom_hidden=mom_hidden, mom_out=mom_out, signs=signs, perturb=perturb, hyper_in=hyper_in, hyper_mid=hyper_mid, hyper_out=hyper_out)


BETA = 0.8
FLOOR = 0.001
SIGMA = 0.01
LR_BASE = 0.03
HIGH = lax.Precision.HIGHEST

def moment_sums(gradient, moment, tensor):
    return jnp.stack([jnp.sum(gradient * gradient), jnp.sum(moment * moment), jnp.sum(tensor * tensor), jnp.sum(gradient * moment)])

def tensor_inputs(sums, step, steps):
    grad_sq = sums[:, 0]
    moment_sq = sums[:, 1]
    weight_sq = sums[:, 2]
    cross_term = sums[:, 3]
    kind_table = jnp.eye(2, dtype=jnp.float32)
    step_share = jnp.full((2,), (step + 1.0) / steps, jnp.float32)
    return jnp.stack([jnp.log(FLOOR + grad_sq), jnp.log(FLOOR + moment_sq), jnp.log(1.0 + weight_sq), cross_term / jnp.sqrt((FLOOR + grad_sq) * (FLOOR + moment_sq)), step_share, jnp.ones((2,), jnp.float32), kind_table[:, 0], kind_table[:, 1]], axis=1)

def apply_rule(tensor, gradient, moment, sums_row, coeffs):
    neurons = (coeffs.shape[0] - 1) // 5
    feat_grad = gradient / jnp.sqrt(FLOOR + sums_row[0])
    feat_moment = moment / jnp.sqrt(FLOOR + sums_row[1])
    direction = jnp.zeros_like(tensor)
    for neuron in range(neurons):
        inner = coeffs[3 * neuron] * feat_grad + coeffs[3 * neuron + 1] * feat_moment + coeffs[3 * neuron + 2] * tensor + coeffs[3 * neurons + neuron]
        direction = direction + coeffs[4 * neurons + neuron] * jnp.maximum(inner, 0.0)
    return tensor - LR_BASE * jnp.exp(coeffs[5 * neurons]) * direction

def reference(inputs, labels, w_hidden, w_out, mom_hidden, mom_out, signs, perturb, hyper_in, hyper_mid, hyper_out):

    def run_task(operands):
        features, classes, hidden_w, out_w, hidden_m, out_m, sign, noise = operands
        theta = hyper_mid + SIGMA * sign.astype(jnp.float32) * noise
        losses = []
        for step in range(STEPS):
            batch_in = features[step]
            hidden_b = hidden_w.astype(jnp.bfloat16)
            out_b = out_w.astype(jnp.bfloat16)
            before = jnp.dot(batch_in, hidden_b, preferred_element_type=jnp.float32) * DIN ** (-0.5)
            active = jnp.maximum(before, 0.0).astype(jnp.bfloat16)
            logits = jnp.dot(active, out_b, preferred_element_type=jnp.float32) * HID ** (-0.5)
            shifted = logits - lax.optimization_barrier(jnp.max(logits, axis=1, keepdims=True))
            log_total = jnp.log(lax.optimization_barrier(jnp.sum(jnp.exp(shifted), axis=1, keepdims=True)))
            onehot = (classes[step][:, None] == jnp.arange(CLASSES, dtype=jnp.int32)[None, :]).astype(jnp.float32)
            example_loss = log_total[:, 0] - lax.optimization_barrier(jnp.sum(shifted * onehot, axis=1))
            losses.append(jnp.sum(example_loss) / BATCH)
            errors = (jnp.exp(shifted - log_total) - onehot).astype(jnp.bfloat16)
            grad_out = jnp.dot(active.T, errors, preferred_element_type=jnp.float32) * HID ** (-0.5)
            back = jnp.dot(errors, out_b.T, preferred_element_type=jnp.float32) * HID ** (-0.5)
            back_pre = jnp.where(before > 0, back, 0.0).astype(jnp.bfloat16)
            grad_hidden = jnp.dot(batch_in.T, back_pre, preferred_element_type=jnp.float32) * DIN ** (-0.5)
            hidden_m = BETA * hidden_m + (1.0 - BETA) * grad_hidden
            out_m = BETA * out_m + (1.0 - BETA) * grad_out
            sums = jnp.stack([moment_sums(grad_hidden, hidden_m, hidden_w) / (DIN * HID), moment_sums(grad_out, out_m, out_w) / (HID * CLASSES)])
            opening = jnp.tanh(jnp.dot(tensor_inputs(sums, step, STEPS), hyper_in, precision=HIGH))
            middle = jnp.tanh(jnp.dot(opening, theta, precision=HIGH))
            coeffs = jnp.dot(middle, hyper_out, precision=HIGH)
            hidden_w = apply_rule(hidden_w, grad_hidden, hidden_m, sums[0], coeffs[0])
            out_w = apply_rule(out_w, grad_out, out_m, sums[1], coeffs[1])
        return (hidden_w, out_w, hidden_m, out_m, jnp.stack(losses))
    new_hidden, new_out, new_mh, new_mo, task_losses = lax.map(run_task, (inputs, labels, w_hidden, w_out, mom_hidden, mom_out, signs, perturb))
    score = lax.optimization_barrier(jnp.sum(task_losses, axis=1)) / STEPS
    center = jnp.sum(score) / TASKS
    weights = signs.astype(jnp.float32) * (score - center) / (SIGMA * TASKS)
    meta_grad = jnp.tensordot(weights, perturb, axes=1, precision=HIGH)
    return (new_hidden, new_out, new_mh, new_mo, task_losses, meta_grad)
```

```python
import jax
import jax.numpy as jnp
from jax import lax
from jax.experimental import pallas as pl
from jax.experimental.pallas import tpu as pltpu
from jax.sharding import PartitionSpec as P

BETA = 0.8
FLOOR = 0.001
SIGMA = 0.01
LR_BASE = 0.03
NEURONS = 4
HIGH = lax.Precision.HIGHEST
BY_ROWS = (((0,), (0,)), ((), ()))
BY_COLUMNS = (((1,), (1,)), ((), ()))
F32 = jnp.float32
BF16 = jnp.bfloat16


def whole(shape):
    return pl.BlockSpec(shape, lambda i: (0,) * len(shape))


def call(kernel, ins, specs, outs, scratch=()):
    return pl.pallas_call(
        kernel,
        grid=(1,),
        in_specs=specs,
        out_specs=[whole(o.shape) for o in outs],
        out_shape=outs,
        scratch_shapes=list(scratch),
        compiler_params=pltpu.CompilerParams(vmem_limit_bytes=56 * 1024 * 1024),
    )(*ins)


def shape_of(shape, dtype=F32):
    return jax.ShapeDtypeStruct(shape, dtype)


def prepare(w_hidden, w_out, mom_hidden, mom_out, signs, perturb, hyper_mid, members):
    rows, width = w_hidden.shape[1:]
    classes = w_out.shape[2]
    trows, hyp = hyper_mid.shape

    def kernel(sign_ref, wh, wo, mh, mo, noise, mid, tensor, moment, send, signed):
        pad = jnp.zeros((rows, width - classes), F32)
        tensor[:, :width] = wh[0]
        tensor[:, width:] = jnp.concatenate([wo[0], pad], axis=1)
        moment[:, :width] = mh[0]
        moment[:, width:] = jnp.concatenate([mo[0], pad], axis=1)
        sign = sign_ref[0].astype(F32)
        signed[...] = sign * noise[0]
        theta = mid[...] + SIGMA * sign * noise[0]
        high = theta.astype(BF16)
        low = (theta - high.astype(F32)).astype(BF16)
        first = tensor[...].astype(BF16)
        for i in range(members):
            send[i, :, : 2 * width] = first
            send[i, :trows, 2 * width :] = high
            send[i, trows:, 2 * width :] = low

    ins = (signs, w_hidden, w_out, mom_hidden, mom_out, perturb, hyper_mid)
    specs = [pl.BlockSpec(memory_space=pltpu.SMEM)] + [whole(a.shape) for a in ins[1:]]
    outs = [
        shape_of((rows, 2 * width)),
        shape_of((rows, 2 * width)),
        shape_of((members, rows, 2 * width + hyp), BF16),
        shape_of((trows, hyp)),
    ]
    return call(kernel, ins, specs, outs)


def forward_backward(inputs, labels, weights, step, classes):
    batch, width_in = inputs.shape[2:]
    width = weights.shape[0]
    scale = width**-0.5
    chunk = batch // 2

    def kernel(x_ref, y_ref, w_ref, g_ref, loss_ref, act_ref, err_ref, dpre_ref):
        loss = jnp.zeros((1, 1), F32)
        for c in range(batch // chunk):
            rows = slice(c * chunk, (c + 1) * chunk)
            before = jnp.dot(x_ref[0, 0, rows, :], w_ref[:, :width], preferred_element_type=F32) * scale
            active = jnp.maximum(before, 0.0).astype(BF16)
            act_ref[rows, :] = active
            logits = jnp.dot(active, w_ref[:, width:], preferred_element_type=F32) * scale
            column = lax.broadcasted_iota(jnp.int32, logits.shape, 1)
            logits = jnp.where(column < classes, logits, -1e30)
            shifted = logits - jnp.max(logits, axis=1, keepdims=True)
            powers = jnp.exp(shifted)
            total = jnp.sum(powers, axis=1, keepdims=True)
            hit = column == y_ref[0, rows, :]
            own = jnp.sum(jnp.where(hit, shifted, 0.0), axis=1, keepdims=True)
            loss = loss + jnp.sum(jnp.log(total) - own, axis=0, keepdims=True)
            errors = (powers * (1.0 / total) - hit.astype(F32)).astype(BF16)
            err_ref[rows, :] = errors
            back = lax.dot_general(errors, w_ref[:, width:], BY_COLUMNS, preferred_element_type=F32) * scale
            dpre_ref[rows, :] = jnp.where(before > 0, back, 0.0).astype(BF16)
        g_ref[:, width:] = lax.dot_general(
            act_ref[...], err_ref[...], BY_ROWS, preferred_element_type=F32
        ).astype(BF16)
        g_ref[:, :width] = lax.dot_general(
            x_ref[0, 0], dpre_ref[...], BY_ROWS, preferred_element_type=F32
        ).astype(BF16)
        place = lax.broadcasted_iota(jnp.int32, (8, 128), 0) + lax.broadcasted_iota(jnp.int32, (8, 128), 1)
        loss_ref[...] = jnp.where(place == 0, jnp.broadcast_to(loss, (8, 128)), 0.0)

    specs = [
        pl.BlockSpec((1, 1, batch, width_in), lambda i: (0, step, 0, 0)),
        pl.BlockSpec((1, batch, 1), lambda i: (step, 0, 0)),
        pl.BlockSpec((width, 2 * width), lambda i: (0, 0)),
    ]
    outs = [shape_of((width, 2 * width), BF16), shape_of((8, 128))]
    scratch = [pltpu.VMEM((batch, width), BF16)] * 3
    return call(kernel, (inputs, labels, weights), specs, outs, scratch)


def reduce_gradient(arrived, moment, tensor, loss, others, width):
    members, rows, both = arrived.shape
    scale = width**-0.5
    block = 16

    def kernel(*refs):
        r_ref, m_ref, p_ref, loss_ref = refs[:4]
        other_refs = refs[4 : 4 + len(others)]
        g_ref, m_out, s_ref = refs[4 + len(others) :]
        totals = [jnp.zeros((8, 128), F32) for _ in range(8)]
        for b in range(rows // block):
            at = slice(b * block, (b + 1) * block)
            for half in range(2):
                for q in range(2):
                    lanes = slice(half * width + q * width // 2, half * width + (q + 1) * width // 2)
                    g = r_ref[0, at, lanes].astype(F32)
                    for i in range(1, members):
                        g = g + r_ref[i, at, lanes].astype(F32)
                    g = g * scale
                    p = p_ref[at, lanes]
                    m = BETA * m_ref[at, lanes] + (1.0 - BETA) * g
                    g_ref[at, lanes] = g
                    m_out[at, lanes] = m
                    for k, product in enumerate((g * g, m * m, p * p, g * m)):
                        part = product[:8] + product[8:]
                        for j in range(width // 256):
                            totals[4 * half + k] = totals[4 * half + k] + part[:, j * 128 : (j + 1) * 128]
        lines = [jnp.sum(t, axis=0, keepdims=True) for t in totals]
        lines.append(loss_ref[0:1, :])
        for ref in other_refs:
            lines.append(ref[0:1, :])
        while len(lines) < 16:
            lines.append(jnp.zeros((1, 128), F32))
        tile = jnp.concatenate(lines, axis=0)
        for i in range(members):
            s_ref[i] = tile

    ins = (arrived, moment, tensor, loss, *others)
    specs = [whole(arrived.shape), whole(moment.shape), whole(tensor.shape), whole(loss.shape)]
    for o in others:
        last = o.shape[0] // 8 - 1
        specs.append(pl.BlockSpec((8, 128), lambda i, last=last: (last, 0)))
    outs = [shape_of((rows, both)), shape_of((rows, both)), shape_of((members, 16, 128))]
    return call(kernel, ins, specs, outs)


def learned_update(sums, sent, hyper_in, hyper_out, gradient, moment, tensor, counts, step, steps, members, classes, last):
    rows, both = gradient.shape
    width = both // 2
    hyp = hyper_in.shape[1]
    half_rows = rows // 2

    def kernel(*refs):
        s_ref, t_ref, in_ref, out_ref, g_ref, m_ref, p_ref = refs[:7]
        total = s_ref[0]
        for i in range(1, members):
            total = total + s_ref[i]
        total = jnp.sum(total, axis=1, keepdims=True)
        means = []
        opening = []
        for k in range(2):
            a, b, c, e = (total[4 * k + j : 4 * k + j + 1, 0:1] / counts[k] for j in range(4))
            means.append((a, b))
            z = (
                jnp.log(FLOOR + a),
                jnp.log(FLOOR + b),
                jnp.log(1.0 + c),
                e / jnp.sqrt((FLOOR + a) * (FLOOR + b)),
            )
            line = in_ref[4:5, :] * ((step + 1.0) / steps) + in_ref[5:6, :] + in_ref[6 + k : 7 + k, :]
            for j in range(4):
                line = line + z[j] * in_ref[j : j + 1, :]
            opening.append(line)
        opening.append(jnp.zeros((6, hyp), F32))
        opening = jnp.tanh(jnp.concatenate(opening, axis=0))
        theta = t_ref[:, :half_rows, :].astype(F32) + t_ref[:, half_rows:, :].astype(F32)
        middle = jnp.tanh(
            jnp.dot(opening, theta.reshape(hyp, hyp), precision=HIGH, preferred_element_type=F32)
        )
        coeffs = jnp.dot(middle, out_ref[...], precision=HIGH, preferred_element_type=F32)
        column = lax.broadcasted_iota(jnp.int32, (1, width), 1)
        for k in range(2):
            g = [coeffs[k : k + 1, j : j + 1] for j in range(5 * NEURONS + 1)]
            by_g = 1.0 / jnp.sqrt(FLOOR + means[k][0])
            by_m = 1.0 / jnp.sqrt(FLOOR + means[k][1])
            rate = LR_BASE * jnp.exp(g[5 * NEURONS])
            lanes = slice(k * width, (k + 1) * width)
            for b in range(rows // 16):
                at = slice(b * 16, (b + 1) * 16)
                f1 = g_ref[at, lanes]
                f2 = m_ref[at, lanes]
                f3 = p_ref[at, lanes]
                direction = jnp.zeros_like(f3)
                for n in range(NEURONS):
                    inner = (
                        (g[3 * n] * by_g) * f1
                        + (g[3 * n + 1] * by_m) * f2
                        + g[3 * n + 2] * f3
                        + g[3 * NEURONS + n]
                    )
                    direction = direction + g[4 * NEURONS + n] * jnp.maximum(inner, 0.0)
                fresh = f3 - rate * direction
                if last is None:
                    if k == 1:
                        fresh = jnp.where(column < classes, fresh, 0.0)
                    refs[7][at, lanes] = fresh
                    for i in range(members):
                        refs[8][i, at, lanes] = fresh.astype(BF16)
                elif k == 0:
                    outs[0][0, at, :] = fresh
                    outs[2][0, at, :] = f2
                else:
                    outs[1][0, at, :] = fresh[:, :classes]
                    outs[3][0, at, :] = f2[:, :classes]

    def final_kernel(*refs):
        nonlocal outs
        signed_refs = refs[7 : 7 + len(last[0])]
        loss_ref = refs[7 + len(last[0])]
        outs = refs[8 + len(last[0]) :]
        kernel(*refs[:7])
        s_ref = refs[0]
        total = s_ref[0]
        for i in range(1, members):
            total = total + s_ref[i]
        total = jnp.sum(total, axis=1, keepdims=True)
        earlier = jnp.sum(loss_ref[...], axis=(0, 1), keepdims=True)
        own = total[8:9, 0:1] / batch_total
        scores = [(earlier + own) / steps]
        for j in range(1, len(signed_refs)):
            scores.append(total[8 + j : 9 + j, 0:1] / batch_total / steps)
        center = scores[0]
        for s in scores[1:]:
            center = center + s
        center = center / len(scores)
        meta = (scores[0] - center) * signed_refs[0][...]
        for s, ref in zip(scores[1:], signed_refs[1:]):
            meta = meta + (s - center) * ref[: meta.shape[0], :]
        outs[4][...] = meta / (SIGMA * len(scores))
        place = lax.broadcasted_iota(jnp.int32, (8, 128), 0) + lax.broadcasted_iota(jnp.int32, (8, 128), 1)
        outs[5][...] = jnp.where(place == 0, jnp.broadcast_to(own, (8, 128)), 0.0)

    def first_kernel(*refs):
        kernel(*refs)
        total = refs[0][0]
        for i in range(1, members):
            total = total + refs[0][i]
        own = jnp.sum(total[8:9, :], axis=1, keepdims=True) / batch_total
        place = lax.broadcasted_iota(jnp.int32, (8, 128), 0) + lax.broadcasted_iota(jnp.int32, (8, 128), 1)
        refs[9][...] = jnp.where(place == 0, jnp.broadcast_to(own, (8, 128)), 0.0)

    outs = None
    batch_total = counts[2]
    ins = [sums, sent, hyper_in, hyper_out, gradient, moment, tensor]
    specs = [whole(a.shape) for a in ins]
    specs[1] = pl.BlockSpec((members, rows, hyp), lambda i: (0, 0, both // hyp))
    if last is None:
        shapes = [shape_of((rows, both)), shape_of((members, rows, both), BF16), shape_of((8, 128))]
        return call(first_kernel, ins, specs, shapes)
    ins = ins + list(last[0]) + [last[1]]
    specs = specs + [whole(a.shape) for a in last[0]] + [whole((8, 128))]
    shapes = [
        shape_of((1, rows, width)),
        shape_of((1, rows, classes)),
        shape_of((1, rows, width)),
        shape_of((1, rows, classes)),
        shape_of(last[0][0].shape),
        shape_of((8, 128)),
    ]
    return call(final_kernel, ins, specs, shapes)


def on_device(
    inputs, labels, w_hidden, w_out, mom_hidden, mom_out, signs, perturb, hyper_in, hyper_mid, hyper_out
):
    members = lax.axis_size("dp")
    tasks = lax.axis_size("task")
    steps, batch, _ = inputs.shape[1:]
    rows, width = w_hidden.shape[1:]
    classes = w_out.shape[2]
    counts = (float(rows * members * width), float(rows * members * classes), float(batch * members))
    label_columns = labels.reshape(steps, batch, 1)
    hyper_out = jnp.pad(hyper_out, ((0, 0), (0, 128 - hyper_out.shape[1])))

    def exchange(copies):
        return lax.all_to_all(copies, "dp", split_axis=0, concat_axis=0, tiled=True)

    tensor, moment, send, signed = prepare(
        w_hidden, w_out, mom_hidden, mom_out, signs, perturb, hyper_mid, members
    )
    weights = exchange(send)
    sent = weights
    local_losses = []
    losses = []
    for step in range(steps):
        partial, loss = forward_backward(
            inputs, label_columns, weights.reshape(rows * members, -1), step, classes
        )
        local_losses.append(loss)
        others = []
        is_last = step == steps - 1
        if is_last:
            tile = jnp.pad(sum(local_losses), ((0, 0), (0, signed.shape[1] - 128)))
            packed = jnp.concatenate([signed, tile], axis=0)
            others = [
                lax.ppermute(packed, "task", [(i, (i + k) % tasks) for i in range(tasks)])
                for k in range(1, tasks)
            ]
        arrived = exchange(partial.reshape(members, rows, 2 * width))
        gradient, moment, sums = reduce_gradient(arrived, moment, tensor, loss, others, width)
        sums = exchange(sums)
        last = ([signed] + others, losses[0]) if is_last else None
        results = learned_update(
            sums, sent, hyper_in, hyper_out, gradient, moment, tensor, counts, step, steps, members, classes, last
        )
        if not is_last:
            tensor, send, loss_tile = results
            losses.append(loss_tile)
            weights = exchange(send)
    new_hidden, new_out, new_mom_hidden, new_mom_out, meta_grad, loss_tile = results
    losses.append(loss_tile)
    loss_row = jnp.stack([tile[0, 0] for tile in losses])[None, :]
    return new_hidden, new_out, new_mom_hidden, new_mom_out, loss_row, meta_grad


def solution(mesh):
    return jax.shard_map(
        on_device,
        mesh=mesh,
        in_specs=(
            P("task", None, "dp", None),
            P("task", None, "dp"),
            P("task", "dp", None),
            P("task", "dp", None),
            P("task", "dp", None),
            P("task", "dp", None),
            P("task"),
            P("task", "dp", None),
            P(),
            P("dp", None),
            P(),
        ),
        out_specs=(
            P("task", "dp", None),
            P("task", "dp", None),
            P("task", "dp", None),
            P("task", "dp", None),
            P("task", None),
            P("dp", None),
        ),
        check_vma=False,
    )
```

```python
import jax
import jax.numpy as jnp
from jax import lax
from jax.experimental import pallas as pl
from jax.experimental.pallas import tpu as pltpu
from jax.sharding import Mesh
from jax.sharding import PartitionSpec as P

BETA = 0.8
FLOOR = 0.001
SIGMA = 0.01
LR_BASE = 0.03
NEURONS = 4
RING = 4
AXES = ("dp_0", "dp_1")
HIGH = lax.Precision.HIGHEST
BY_ROWS = (((0,), (0,)), ((), ()))
BY_COLUMNS = (((1,), (1,)), ((), ()))
F32 = jnp.float32
BF16 = jnp.bfloat16


VMEM = pl.BlockSpec(memory_space=pltpu.VMEM)
SMEM = pl.BlockSpec(memory_space=pltpu.SMEM)


def call(kernel, ins, outs, scratch=(), scalars=0):
    return pl.pallas_call(
        kernel,
        in_specs=[SMEM] * scalars + [VMEM] * (len(ins) - scalars),
        out_specs=[VMEM] * len(outs),
        out_shape=outs,
        scratch_shapes=list(scratch),
        compiler_params=pltpu.CompilerParams(vmem_limit_bytes=30 * 1024 * 1024),
    )(*ins)


def shape_of(shape, dtype=F32):
    return jax.ShapeDtypeStruct(shape, dtype)


def prepare(w_hidden, w_out, mom_hidden, mom_out, signs, perturb, hyper_mid):
    rows, width = w_hidden.shape[1:]
    classes = w_out.shape[2]
    trows, hyp = hyper_mid.shape
    half = hyp // 2

    def kernel(sign_ref, wh, wo, mh, mo, noise, mid, tensor, moment, send_a, send_b, signed):
        pad = jnp.zeros((rows, width - classes), F32)
        tensor[:, :width] = wh[0]
        tensor[:, width:] = jnp.concatenate([wo[0], pad], axis=1)
        moment[:, :width] = mh[0]
        moment[:, width:] = jnp.concatenate([mo[0], pad], axis=1)
        sign = sign_ref[0].astype(F32)
        signed[...] = sign * noise[0]
        theta = mid[...] + SIGMA * sign * noise[0]
        high = theta.astype(BF16)
        low = (theta - high.astype(F32)).astype(BF16)
        for ref, lanes, extra in ((send_a, slice(0, width), high), (send_b, slice(width, 2 * width), low)):
            ref[:, :width] = tensor[:, lanes].astype(BF16)
            ref[:trows, width:] = extra[:, :half]
            ref[trows:, width:] = extra[:, half:]

    outs = [
        shape_of((rows, 2 * width)),
        shape_of((rows, 2 * width)),
        shape_of((rows, width + half), BF16),
        shape_of((rows, width + half), BF16),
        shape_of((trows, hyp)),
    ]
    return call(kernel, (signs, w_hidden, w_out, mom_hidden, mom_out, perturb, hyper_mid), outs, scalars=1)


def turned(place, k):
    return lax.rem(place + (RING - k), RING)


def shifted_copies(arrays, axis):
    return [
        lax.ppermute(a, axis, [(i, (i + k) % RING) for i in range(RING)])
        for k, a in enumerate(arrays, 1)
    ]


def gathered(place, send_a, send_b):
    rows, width = send_a.shape
    from_a = [send_a] + shifted_copies([send_a] * 3, AXES[1])
    from_b = [send_b] + shifted_copies([send_b] * 3, AXES[0])

    def kernel(place_ref, *refs):
        for k in range(RING):
            refs[8][turned(place_ref[1], k)] = refs[k][...]
            refs[9][turned(place_ref[0], k)] = refs[4 + k][...]

    four_a, four_b = call(
        kernel, (place, *from_a, *from_b), [shape_of((RING, rows, width), BF16)] * 2, scalars=1
    )
    return (
        [four_a] + shifted_copies([four_a] * 3, AXES[0]),
        [four_b] + shifted_copies([four_b] * 3, AXES[1]),
    )


def joined_theta(place, all_a, all_b, width, trows):
    half = all_a[0].shape[2] - width

    def kernel(place_ref, *refs):
        out = refs[8]
        for k in range(RING):
            z = turned(place_ref[0], k)
            for j in range(RING):
                out[z * RING + j, :, :half] = refs[k][j, :trows, width:].astype(F32)
                out[z * RING + j, :, half:] = refs[k][j, trows:, width:].astype(F32)
        for k in range(RING):
            y = turned(place_ref[1], k)
            for j in range(RING):
                at = j * RING + y
                out[at, :, :half] = out[at, :, :half] + refs[4 + k][j, :trows, width:].astype(F32)
                out[at, :, half:] = out[at, :, half:] + refs[4 + k][j, trows:, width:].astype(F32)

    (theta,) = call(
        kernel, (place, *all_a, *all_b), [shape_of((RING * RING, trows, 2 * half))], scalars=1
    )
    return theta


def forward_backward(place, inputs, labels, all_a, all_b, step, classes):
    batch, width = inputs.shape[2:]
    rows = all_a[0].shape[1]
    slab = RING * rows
    scale = width**-0.5
    chunk = batch // 2

    def kernel(place_ref, x_ref, y_ref, *refs):
        a_refs, b_refs = refs[:4], refs[4:8]
        g1_refs, g2_refs, loss_ref = refs[8:12], refs[12:16], refs[16]
        w1_ref, w2_ref, act_ref, err_ref, dpre_ref, g_ref = refs[17:]
        for k in range(RING):
            at = pl.multiple_of(turned(place_ref[0], k) * slab, slab)
            y = turned(place_ref[1], k)
            for j in range(RING):
                w1_ref[pl.ds(at + j * rows, rows), :] = a_refs[k][j, :, :width]
                w2_ref[pl.ds(pl.multiple_of(j * slab + y * rows, rows), rows), :] = b_refs[k][j, :, :width]
        loss = jnp.zeros((1, 1), F32)
        for c in range(batch // chunk):
            part = slice(c * chunk, (c + 1) * chunk)
            before = jnp.dot(x_ref[0, step, part, :], w1_ref[...], preferred_element_type=F32) * scale
            active = jnp.maximum(before, 0.0).astype(BF16)
            act_ref[part, :] = active
            logits = jnp.dot(active, w2_ref[...], preferred_element_type=F32) * scale
            column = lax.broadcasted_iota(jnp.int32, logits.shape, 1)
            logits = jnp.where(column < classes, logits, -1e30)
            shifted = logits - jnp.max(logits, axis=1, keepdims=True)
            powers = jnp.exp(shifted)
            total = jnp.sum(powers, axis=1, keepdims=True)
            hit = column == y_ref[step, part, :]
            own = jnp.sum(jnp.where(hit, shifted, 0.0), axis=1, keepdims=True)
            loss = loss + jnp.sum(jnp.log(total) - own, axis=0, keepdims=True)
            errors = (powers * (1.0 / total) - hit.astype(F32)).astype(BF16)
            err_ref[part, :] = errors
            back = lax.dot_general(errors, w2_ref[...], BY_COLUMNS, preferred_element_type=F32) * scale
            dpre_ref[part, :] = jnp.where(before > 0, back, 0.0).astype(BF16)
        g_ref[...] = lax.dot_general(
            act_ref[...], err_ref[...], BY_ROWS, preferred_element_type=F32
        ).astype(BF16)
        for k in range(RING):
            y = lax.rem(place_ref[1] + k, RING)
            for j in range(RING):
                g2_refs[k][j] = g_ref[pl.ds(pl.multiple_of(j * slab + y * rows, rows), rows), :]
        g_ref[...] = lax.dot_general(
            x_ref[0, step], dpre_ref[...], BY_ROWS, preferred_element_type=F32
        ).astype(BF16)
        for k in range(RING):
            at = pl.multiple_of(lax.rem(place_ref[0] + k, RING) * slab, slab)
            for j in range(RING):
                g1_refs[k][j] = g_ref[pl.ds(at + j * rows, rows), :]
        spot = lax.broadcasted_iota(jnp.int32, (8, 128), 0) + lax.broadcasted_iota(jnp.int32, (8, 128), 1)
        loss_ref[...] = jnp.where(spot == 0, jnp.broadcast_to(loss, (8, 128)), 0.0)

    outs = [shape_of((RING, rows, width), BF16)] * 8 + [shape_of((8, 128))]
    scratch = [pltpu.VMEM((width, width), BF16)] * 2 + [pltpu.VMEM((batch, width), BF16)] * 3
    scratch = scratch + [pltpu.VMEM((width, width), BF16)]
    results = call(kernel, (place, inputs, labels, *all_a, *all_b), outs, scratch, scalars=1)
    return results[:4], results[4:8], results[8]


def scattered(place, first, second):
    rows, width = first[0].shape[1:]
    first = [first[0]] + shifted_copies(first[1:], AXES[0])
    second = [second[0]] + shifted_copies(second[1:], AXES[1])

    def kernel(place_ref, *refs):
        for axis, ins, outs in ((1, refs[:4], refs[8:12]), (0, refs[4:8], refs[12:16])):
            for k in range(RING):
                at = lax.rem(place_ref[axis] + k, RING)
                total = ins[0][at].astype(F32)
                for i in range(1, RING):
                    total = total + ins[i][at].astype(F32)
                outs[k][...] = total.astype(outs[k].dtype)

    outs = ([shape_of((rows, width))] + [shape_of((rows, width), BF16)] * 3) * 2
    parts = call(kernel, (place, *first, *second), outs, scalars=1)
    return (
        [parts[0]] + shifted_copies(parts[1:4], AXES[1]),
        [parts[4]] + shifted_copies(parts[5:8], AXES[0]),
    )


def reduce_gradient(parts, moment, tensor, loss, others, members):
    rows, both = moment.shape
    width = both // 2
    scale = width**-0.5
    block = 16

    def kernel(*refs):
        r_refs, refs = refs[:8], refs[8:]
        m_ref, p_ref, loss_ref = refs[:3]
        other_refs = refs[3 : 3 + len(others)]
        g_ref, m_out, s_ref = refs[3 + len(others) :]
        totals = [jnp.zeros((8, 128), F32) for _ in range(8)]
        for b in range(rows // block):
            at = slice(b * block, (b + 1) * block)
            for half in range(2):
                for q in range(2):
                    lanes = slice(half * width + q * width // 2, half * width + (q + 1) * width // 2)
                    own = slice(q * width // 2, (q + 1) * width // 2)
                    g = r_refs[4 * half][at, own]
                    for i in range(1, RING):
                        g = g + r_refs[4 * half + i][at, own].astype(F32)
                    g = g * scale
                    p = p_ref[at, lanes]
                    m = BETA * m_ref[at, lanes] + (1.0 - BETA) * g
                    g_ref[at, lanes] = g
                    m_out[at, lanes] = m
                    for k, product in enumerate((g * g, m * m, p * p, g * m)):
                        part = product[:8] + product[8:]
                        for j in range(width // 256):
                            totals[4 * half + k] = totals[4 * half + k] + part[:, j * 128 : (j + 1) * 128]
        lines = [jnp.sum(t, axis=0, keepdims=True) for t in totals]
        lines.append(loss_ref[0:1, :])
        for ref in other_refs:
            lines.append(ref[ref.shape[0] - 8 : ref.shape[0] - 7, :128])
        while len(lines) < 16:
            lines.append(jnp.zeros((1, 128), F32))
        tile = jnp.concatenate(lines, axis=0)
        for i in range(members):
            s_ref[i] = tile

    ins = (*parts[0], *parts[1], moment, tensor, loss, *others)
    outs = [shape_of((rows, both)), shape_of((rows, both)), shape_of((members, 16, 128))]
    return call(kernel, ins, outs)


def learned_update(sums, theta, hyper_in, hyper_out, gradient, moment, tensor, counts, step, steps, members, classes, last):
    rows, both = gradient.shape
    width = both // 2
    hyp = hyper_in.shape[1]

    def kernel(*refs):
        s_ref, t_ref, in_ref, out_ref, g_ref, m_ref, p_ref = refs[:7]
        total = s_ref[0]
        for i in range(1, members):
            total = total + s_ref[i]
        total = jnp.sum(total, axis=1, keepdims=True)
        means = []
        opening = []
        for k in range(2):
            a, b, c, e = (total[4 * k + j : 4 * k + j + 1, 0:1] / counts[k] for j in range(4))
            means.append((a, b))
            z = (
                jnp.log(FLOOR + a),
                jnp.log(FLOOR + b),
                jnp.log(1.0 + c),
                e / jnp.sqrt((FLOOR + a) * (FLOOR + b)),
            )
            line = in_ref[4:5, :] * ((step + 1.0) / steps) + in_ref[5:6, :] + in_ref[6 + k : 7 + k, :]
            for j in range(4):
                line = line + z[j] * in_ref[j : j + 1, :]
            opening.append(line)
        opening.append(jnp.zeros((6, hyp), F32))
        opening = jnp.tanh(jnp.concatenate(opening, axis=0))
        middle = jnp.tanh(
            jnp.dot(opening, t_ref[...].reshape(hyp, hyp), precision=HIGH, preferred_element_type=F32)
        )
        coeffs = jnp.dot(middle, out_ref[...], precision=HIGH, preferred_element_type=F32)
        column = lax.broadcasted_iota(jnp.int32, (1, width), 1)
        for k in range(2):
            g = [coeffs[k : k + 1, j : j + 1] for j in range(5 * NEURONS + 1)]
            by_g = 1.0 / jnp.sqrt(FLOOR + means[k][0])
            by_m = 1.0 / jnp.sqrt(FLOOR + means[k][1])
            rate = LR_BASE * jnp.exp(g[5 * NEURONS])
            lanes = slice(k * width, (k + 1) * width)
            for b in range(rows // 16):
                at = slice(b * 16, (b + 1) * 16)
                f1 = g_ref[at, lanes]
                f2 = m_ref[at, lanes]
                f3 = p_ref[at, lanes]
                direction = jnp.zeros_like(f3)
                for n in range(NEURONS):
                    inner = (
                        (g[3 * n] * by_g) * f1
                        + (g[3 * n + 1] * by_m) * f2
                        + g[3 * n + 2] * f3
                        + g[3 * NEURONS + n]
                    )
                    direction = direction + g[4 * NEURONS + n] * jnp.maximum(inner, 0.0)
                fresh = f3 - rate * direction
                if last is None:
                    if k == 1:
                        fresh = jnp.where(column < classes, fresh, 0.0)
                    refs[7][at, lanes] = fresh
                    refs[8 + k][at, :] = fresh.astype(BF16)
                elif k == 0:
                    outs[0][0, at, :] = fresh
                    outs[2][0, at, :] = f2
                else:
                    outs[1][0, at, :] = fresh[:, :classes]
                    outs[3][0, at, :] = f2[:, :classes]

    def final_kernel(*refs):
        nonlocal outs
        signed_refs = refs[7 : 7 + len(last[0])]
        loss_ref = refs[7 + len(last[0])]
        outs = refs[8 + len(last[0]) :]
        kernel(*refs[:7])
        s_ref = refs[0]
        total = s_ref[0]
        for i in range(1, members):
            total = total + s_ref[i]
        total = jnp.sum(total, axis=1, keepdims=True)
        earlier = jnp.sum(loss_ref[...], axis=(0, 1), keepdims=True)
        own = total[8:9, 0:1] / batch_total
        scores = [(earlier + own) / steps]
        for j in range(1, len(signed_refs)):
            scores.append(total[8 + j : 9 + j, 0:1] / batch_total / steps)
        center = scores[0]
        for s in scores[1:]:
            center = center + s
        center = center / len(scores)
        meta = (scores[0] - center) * signed_refs[0][...]
        for s, ref in zip(scores[1:], signed_refs[1:]):
            meta = meta + (s - center) * ref[: meta.shape[0], :]
        outs[4][...] = meta / (SIGMA * len(scores))
        place = lax.broadcasted_iota(jnp.int32, (8, 128), 0) + lax.broadcasted_iota(jnp.int32, (8, 128), 1)
        outs[5][...] = jnp.where(place == 0, jnp.broadcast_to(own, (8, 128)), 0.0)

    def first_kernel(*refs):
        kernel(*refs)
        total = refs[0][0]
        for i in range(1, members):
            total = total + refs[0][i]
        own = jnp.sum(total[8:9, :], axis=1, keepdims=True) / batch_total
        place = lax.broadcasted_iota(jnp.int32, (8, 128), 0) + lax.broadcasted_iota(jnp.int32, (8, 128), 1)
        refs[10][...] = jnp.where(place == 0, jnp.broadcast_to(own, (8, 128)), 0.0)

    outs = None
    batch_total = counts[2]
    ins = [sums, theta, hyper_in, hyper_out, gradient, moment, tensor]
    if last is None:
        shapes = [shape_of((rows, both))] + [shape_of((rows, width), BF16)] * 2 + [shape_of((8, 128))]
        return call(first_kernel, ins, shapes)
    ins = ins + list(last[0]) + [last[1]]
    shapes = [
        shape_of((1, rows, width)),
        shape_of((1, rows, classes)),
        shape_of((1, rows, width)),
        shape_of((1, rows, classes)),
        shape_of(last[0][0].shape),
        shape_of((8, 128)),
    ]
    return call(final_kernel, ins, shapes)


def on_device(
    inputs, labels, w_hidden, w_out, mom_hidden, mom_out, signs, perturb, hyper_in, hyper_mid, hyper_out
):
    members = lax.axis_size(AXES)
    tasks = lax.axis_size("task")
    steps, batch, _ = inputs.shape[1:]
    rows, width = w_hidden.shape[1:]
    classes = w_out.shape[2]
    counts = (float(rows * members * width), float(rows * members * classes), float(batch * members))
    label_columns = labels.reshape(steps, batch, 1)
    hyper_out = jnp.pad(hyper_out, ((0, 0), (0, 128 - hyper_out.shape[1])))

    place = jnp.stack([lax.axis_index(axis) for axis in AXES]).astype(jnp.int32)
    tensor, moment, send_a, send_b, signed = prepare(
        w_hidden, w_out, mom_hidden, mom_out, signs, perturb, hyper_mid
    )
    theta = None
    local_losses = []
    losses = []
    for step in range(steps):
        all_a, all_b = gathered(place, send_a, send_b)
        if theta is None:
            theta = joined_theta(place, all_a, all_b, width, hyper_mid.shape[0])
        first, second, loss = forward_backward(place, inputs, label_columns, all_a, all_b, step, classes)
        local_losses.append(loss)
        others = []
        is_last = step == steps - 1
        if is_last:
            tile = jnp.pad(sum(local_losses), ((0, 0), (0, signed.shape[1] - 128)))
            packed = jnp.concatenate([signed, tile], axis=0)
            others = [
                lax.ppermute(packed, "task", [(i, (i + k) % tasks) for i in range(tasks)])
                for k in range(1, tasks)
            ]
        parts = scattered(place, first, second)
        gradient, moment, sums = reduce_gradient(parts, moment, tensor, loss, others, members)
        sums = lax.all_to_all(sums, AXES, split_axis=0, concat_axis=0, tiled=True)
        last = ([signed] + others, losses[0]) if is_last else None
        results = learned_update(
            sums, theta, hyper_in, hyper_out, gradient, moment, tensor, counts, step, steps, members, classes, last
        )
        if not is_last:
            tensor, send_a, send_b, loss_tile = results
            losses.append(loss_tile)
    new_hidden, new_out, new_mom_hidden, new_mom_out, meta_grad, loss_tile = results
    losses.append(loss_tile)
    loss_row = jnp.stack([tile[0, 0] for tile in losses])[None, :]
    return new_hidden, new_out, new_mom_hidden, new_mom_out, loss_row, meta_grad


def solution(mesh):
    split = Mesh(mesh.devices.reshape(mesh.shape["task"], RING, RING), ("task", *AXES))
    return jax.shard_map(
        on_device,
        mesh=split,
        in_specs=(
            P("task", None, AXES, None),
            P("task", None, AXES),
            P("task", AXES, None),
            P("task", AXES, None),
            P("task", AXES, None),
            P("task", AXES, None),
            P("task"),
            P("task", AXES, None),
            P(),
            P(AXES, None),
            P(),
        ),
        out_specs=(
            P("task", AXES, None),
            P("task", AXES, None),
            P("task", AXES, None),
            P("task", AXES, None),
            P("task", None),
            P(AXES, None),
        ),
        check_vma=False,
    )
```

```python
import jax
import jax.numpy as jnp
from jax import lax
from jax.experimental import pallas as pl
from jax.experimental.pallas import tpu as pltpu
from jax.sharding import Mesh
from jax.sharding import PartitionSpec as P

BETA = 0.8
FLOOR = 0.001
SIGMA = 0.01
LR_BASE = 0.03
NEURONS = 4
RING = 4
LINES = 24
AXES = ("dp_0", "dp_1")
HIGH = lax.Precision.HIGHEST
BY_ROWS = (((0,), (0,)), ((), ()))
BY_COLUMNS = (((1,), (1,)), ((), ()))
F32 = jnp.float32
BF16 = jnp.bfloat16


VMEM = pl.BlockSpec(memory_space=pltpu.VMEM)
ANY = pl.BlockSpec(memory_space=pl.ANY)
SMEM = pl.BlockSpec(memory_space=pltpu.SMEM)


def call(kernel, ins, outs, scratch=(), scalars=0, space=VMEM):
    return pl.pallas_call(
        kernel,
        in_specs=[SMEM] * scalars + [space] * (len(ins) - scalars),
        out_specs=[VMEM] * len(outs),
        out_shape=outs,
        scratch_shapes=list(scratch),
        compiler_params=pltpu.CompilerParams(vmem_limit_bytes=30 * 1024 * 1024),
    )(*ins)


def shape_of(shape, dtype=F32):
    return jax.ShapeDtypeStruct(shape, dtype)


def fetch(pairs, sems):
    copies = [pltpu.make_async_copy(src, dst, sems.at[i]) for i, (src, dst) in enumerate(pairs)]
    for copy in copies:
        copy.start()
    return copies


def prepare(w_hidden, w_out, signs, perturb, hyper_mid):
    rows, width = w_hidden.shape[1:]
    classes = w_out.shape[2]
    trows, hyp = hyper_mid.shape
    half = hyp // 2

    def kernel(sign_ref, wh_any, wo_any, noise_any, mid_any, send_a, send_b, signed, wh, wo, noise, mid, sems):
        copies = fetch(((wh_any, wh), (wo_any, wo), (noise_any, noise), (mid_any, mid)), sems)
        copies[0].wait()
        send_a[:, :width] = wh[0].astype(BF16)
        copies[1].wait()
        pad = jnp.zeros((rows, width - classes), F32)
        send_b[:, :width] = jnp.concatenate([wo[0], pad], axis=1).astype(BF16)
        copies[2].wait()
        copies[3].wait()
        sign = sign_ref[0].astype(F32)
        signed[...] = sign * noise[0]
        theta = mid[...] + SIGMA * sign * noise[0]
        high = theta.astype(BF16)
        low = (theta - high.astype(F32)).astype(BF16)
        for ref, extra in ((send_a, high), (send_b, low)):
            ref[:trows, width:] = extra[:, :half]
            ref[trows:, width:] = extra[:, half:]

    outs = [
        shape_of((rows, width + half), BF16),
        shape_of((rows, width + half), BF16),
        shape_of((trows, hyp)),
    ]
    ins = (signs, w_hidden, w_out, perturb, hyper_mid)
    scratch = [pltpu.VMEM(a.shape, F32) for a in ins[1:]] + [pltpu.SemaphoreType.DMA((4,))]
    return call(kernel, ins, outs, scratch, scalars=1, space=ANY)


def side_by_side(w_hidden, w_out, mom_hidden, mom_out, after):
    rows, width = w_hidden.shape[1:]
    classes = w_out.shape[2]

    def kernel(wh_any, wo_any, mh_any, mo_any, _, tensor, moment, wh, wo, mh, mo, sems):
        pairs = ((wh_any, wh), (wo_any, wo), (mh_any, mh), (mo_any, mo))
        for copy in fetch(pairs, sems):
            copy.wait()
        pad = jnp.zeros((rows, width - classes), F32)
        tensor[:, :width] = wh[0]
        tensor[:, width:] = jnp.concatenate([wo[0], pad], axis=1)
        moment[:, :width] = mh[0]
        moment[:, width:] = jnp.concatenate([mo[0], pad], axis=1)

    ins = (w_hidden, w_out, mom_hidden, mom_out, after)
    scratch = [pltpu.VMEM(a.shape, F32) for a in ins[:4]] + [pltpu.SemaphoreType.DMA((4,))]
    return call(kernel, ins, [shape_of((rows, 2 * width))] * 2, scratch, space=ANY)


def packed_copies(signed, losses, tasks):
    trows, hyp = signed.shape

    def kernel(*refs):
        out = refs[-1]
        total = refs[1][...]
        for ref in refs[2:-1]:
            total = total + ref[...]
        for t in range(tasks):
            out[t, :trows, :] = refs[0][...]
            out[t, trows:, :128] = total
            out[t, trows:, 128:] = jnp.zeros((8, hyp - 128), F32)

    return call(kernel, (signed, *losses), [shape_of((tasks, trows + 8, hyp))])[0]


def turned(place, k):
    return lax.rem(place + (RING - k), RING)


def shifted_copies(first, first_axis, second, second_axis):
    got = {}
    for k in (1, 3, 2):
        pairs = [(i, (i + k) % RING) for i in range(RING)]
        got[0, k] = lax.ppermute(first[k], first_axis, pairs)
        got[1, k] = lax.ppermute(second[k], second_axis, pairs)
    return (
        [first[0]] + [got[0, k] for k in range(1, RING)],
        [second[0]] + [got[1, k] for k in range(1, RING)],
    )


def gathered(place, send_a, send_b):
    rows, width = send_a.shape
    from_a, from_b = shifted_copies([send_a] * RING, AXES[1], [send_b] * RING, AXES[0])

    def kernel(place_ref, *refs):
        for k in range(RING):
            refs[8][turned(place_ref[1], k)] = refs[k][...]
            refs[9][turned(place_ref[0], k)] = refs[4 + k][...]

    four_a, four_b = call(
        kernel, (place, *from_a, *from_b), [shape_of((RING, rows, width), BF16)] * 2, scalars=1
    )
    all_a, all_b = shifted_copies([four_a] * RING, AXES[0], [four_b] * RING, AXES[1])
    return all_a, all_b, from_a[1]


def joined_theta(place, all_a, all_b, width, trows):
    half = all_a[0].shape[2] - width

    def kernel(place_ref, *refs):
        out = refs[8]
        for k in range(RING):
            z = turned(place_ref[0], k)
            for j in range(RING):
                out[z * RING + j, :, :half] = refs[k][j, :trows, width:].astype(F32)
                out[z * RING + j, :, half:] = refs[k][j, trows:, width:].astype(F32)
        for k in range(RING):
            y = turned(place_ref[1], k)
            for j in range(RING):
                at = j * RING + y
                out[at, :, :half] = out[at, :, :half] + refs[4 + k][j, :trows, width:].astype(F32)
                out[at, :, half:] = out[at, :, half:] + refs[4 + k][j, trows:, width:].astype(F32)

    (theta,) = call(
        kernel, (place, *all_a, *all_b), [shape_of((RING * RING, trows, 2 * half))], scalars=1
    )
    return theta


def forward_backward(place, inputs, labels, all_a, all_b, step, classes):
    batch, width = inputs.shape[2:]
    rows = all_a[0].shape[1]
    slab = RING * rows
    scale = width**-0.5
    chunk = batch // 2

    def kernel(place_ref, x_ref, y_ref, *refs):
        a_refs, b_refs = refs[:4], refs[4:8]
        g1_refs, g2_refs, loss_ref = refs[8:12], refs[12:16], refs[16]
        w1_ref, w2_ref, act_ref, err_ref, dpre_ref, g_ref = refs[17:]
        def place_weights(j, _):
            for k in range(RING):
                at = turned(place_ref[0], k) * slab + j * rows
                w1_ref[pl.ds(pl.multiple_of(at, rows), rows), :] = a_refs[k][j, :, :width]
                at = j * slab + turned(place_ref[1], k) * rows
                w2_ref[pl.ds(pl.multiple_of(at, rows), rows), :] = b_refs[k][j, :, :width]

        lax.fori_loop(0, RING, place_weights, None)
        loss = jnp.zeros((1, 1), F32)
        for c in range(batch // chunk):
            part = slice(c * chunk, (c + 1) * chunk)
            before = jnp.dot(x_ref[0, step, part, :], w1_ref[...], preferred_element_type=F32) * scale
            active = jnp.maximum(before, 0.0).astype(BF16)
            act_ref[part, :] = active
            logits = jnp.dot(active, w2_ref[...], preferred_element_type=F32) * scale
            column = lax.broadcasted_iota(jnp.int32, logits.shape, 1)
            logits = jnp.where(column < classes, logits, -1e30)
            shifted = logits - jnp.max(logits, axis=1, keepdims=True)
            powers = jnp.exp(shifted)
            total = jnp.sum(powers, axis=1, keepdims=True)
            hit = column == y_ref[step, part, :]
            own = jnp.sum(jnp.where(hit, shifted, 0.0), axis=1, keepdims=True)
            loss = loss + jnp.sum(jnp.log(total) - own, axis=0, keepdims=True)
            errors = (powers * (1.0 / total) - hit.astype(F32)).astype(BF16)
            err_ref[part, :] = errors
            back = lax.dot_general(errors, w2_ref[...], BY_COLUMNS, preferred_element_type=F32) * scale
            dpre_ref[part, :] = jnp.where(before > 0, back, 0.0).astype(BF16)
        g_ref[...] = lax.dot_general(
            act_ref[...], err_ref[...], BY_ROWS, preferred_element_type=F32
        ).astype(BF16)

        def cut_second(j, _):
            for k in range(RING):
                at = j * slab + lax.rem(place_ref[1] + k, RING) * rows
                g2_refs[k][j] = g_ref[pl.ds(pl.multiple_of(at, rows), rows), :]

        lax.fori_loop(0, RING, cut_second, None)
        g_ref[...] = lax.dot_general(
            x_ref[0, step], dpre_ref[...], BY_ROWS, preferred_element_type=F32
        ).astype(BF16)

        def cut_first(j, _):
            for k in range(RING):
                at = lax.rem(place_ref[0] + k, RING) * slab + j * rows
                g1_refs[k][j] = g_ref[pl.ds(pl.multiple_of(at, rows), rows), :]

        lax.fori_loop(0, RING, cut_first, None)
        spot = lax.broadcasted_iota(jnp.int32, (8, 128), 0) + lax.broadcasted_iota(jnp.int32, (8, 128), 1)
        loss_ref[...] = jnp.where(spot == 0, jnp.broadcast_to(loss, (8, 128)), 0.0)

    outs = [shape_of((RING, rows, width), BF16)] * 8 + [shape_of((8, 128))]
    scratch = [pltpu.VMEM((width, width), BF16)] * 2 + [pltpu.VMEM((batch, width), BF16)] * 3
    scratch = scratch + [pltpu.VMEM((width, width), BF16)]
    results = call(kernel, (place, inputs, labels, *all_a, *all_b), outs, scratch, scalars=1)
    return results[:4], results[4:8], results[8]


def scattered(place, first, second, after):
    rows, width = first[0].shape[1:]
    first, second = shifted_copies(first, AXES[0], second, AXES[1])

    def kernel(place_ref, *refs):
        outs = refs[-8:]

        def block(b, _):
            lines = pl.ds(pl.multiple_of(b * 16, 16), 16)
            for axis, ins, own in ((1, refs[:4], outs[:4]), (0, refs[4:8], outs[4:])):
                for k in range(RING):
                    at = lax.rem(place_ref[axis] + k, RING)
                    total = ins[0][at, lines, :].astype(F32)
                    for i in range(1, RING):
                        total = total + ins[i][at, lines, :].astype(F32)
                    own[k][lines, :] = total.astype(own[k].dtype)

        lax.fori_loop(0, rows // 16, block, None)

    outs = ([shape_of((rows, width))] + [shape_of((rows, width), BF16)] * 3) * 2
    parts = call(kernel, (place, *first, *second, *after), outs, scalars=1)
    return shifted_copies(parts[:4], AXES[1], parts[4:], AXES[0])


def reduce_gradient(parts, moment, tensor, loss, others, members):
    rows, both = moment.shape
    width = both // 2
    scale = width**-0.5
    block = 16

    def kernel(*refs):
        r_refs, refs = refs[:8], refs[8:]
        m_ref, p_ref, loss_ref = refs[:3]
        other_refs = refs[3 : 3 + len(others)]
        g_ref, m_out, s_ref = refs[3 + len(others) :]
        totals = [jnp.zeros((8, 128), F32) for _ in range(8)]
        for b in range(rows // block):
            at = slice(b * block, (b + 1) * block)
            for half in range(2):
                for q in range(2):
                    lanes = slice(half * width + q * width // 2, half * width + (q + 1) * width // 2)
                    own = slice(q * width // 2, (q + 1) * width // 2)
                    g = r_refs[4 * half][at, own]
                    for i in range(1, RING):
                        g = g + r_refs[4 * half + i][at, own].astype(F32)
                    g = g * scale
                    p = p_ref[at, lanes]
                    m = BETA * m_ref[at, lanes] + (1.0 - BETA) * g
                    g_ref[at, lanes] = g
                    m_out[at, lanes] = m
                    for k, product in enumerate((g * g, m * m, p * p, g * m)):
                        part = product[:8] + product[8:]
                        for j in range(width // 256):
                            totals[4 * half + k] = totals[4 * half + k] + part[:, j * 128 : (j + 1) * 128]
        lines = [jnp.sum(t, axis=0, keepdims=True) for t in totals]
        lines.append(loss_ref[0:1, :])
        for ref in other_refs:
            for t in range(ref.shape[0]):
                lines.append(ref[t, ref.shape[1] - 8 : ref.shape[1] - 7, :128])
        while len(lines) < LINES:
            lines.append(jnp.zeros((1, 128), F32))
        tile = jnp.concatenate(lines, axis=0)
        for i in range(members):
            s_ref[i] = tile

    ins = (*parts[0], *parts[1], moment, tensor, loss, *others)
    outs = [shape_of((rows, both)), shape_of((rows, both)), shape_of((members, LINES, 128))]
    return call(kernel, ins, outs)


def learned_update(sums, theta, hyper_in, hyper_out, gradient, moment, tensor, counts, step, steps, members, classes, last):
    rows, both = gradient.shape
    width = both // 2
    hyp = hyper_in.shape[1]

    def kernel(*refs):
        s_ref, t_ref, in_ref, out_ref, g_ref, m_ref, p_ref = refs[:7]
        total = s_ref[0]
        for i in range(1, members):
            total = total + s_ref[i]
        total = jnp.sum(total, axis=1, keepdims=True)
        means = []
        opening = []
        for k in range(2):
            a, b, c, e = (total[4 * k + j : 4 * k + j + 1, 0:1] / counts[k] for j in range(4))
            means.append((a, b))
            z = (
                jnp.log(FLOOR + a),
                jnp.log(FLOOR + b),
                jnp.log(1.0 + c),
                e / jnp.sqrt((FLOOR + a) * (FLOOR + b)),
            )
            line = in_ref[4:5, :] * ((step + 1.0) / steps) + in_ref[5:6, :] + in_ref[6 + k : 7 + k, :]
            for j in range(4):
                line = line + z[j] * in_ref[j : j + 1, :]
            opening.append(line)
        opening.append(jnp.zeros((6, hyp), F32))
        opening = jnp.tanh(jnp.concatenate(opening, axis=0))
        middle = jnp.tanh(
            jnp.dot(opening, t_ref[...].reshape(hyp, hyp), precision=HIGH, preferred_element_type=F32)
        )
        coeffs = jnp.dot(middle, out_ref[...], precision=HIGH, preferred_element_type=F32)
        column = lax.broadcasted_iota(jnp.int32, (1, width), 1)
        for k in range(2):
            g = [coeffs[k : k + 1, j : j + 1] for j in range(5 * NEURONS + 1)]
            by_g = 1.0 / jnp.sqrt(FLOOR + means[k][0])
            by_m = 1.0 / jnp.sqrt(FLOOR + means[k][1])
            rate = LR_BASE * jnp.exp(g[5 * NEURONS])
            lanes = slice(k * width, (k + 1) * width)
            for b in range(rows // 16):
                at = slice(b * 16, (b + 1) * 16)
                f1 = g_ref[at, lanes]
                f2 = m_ref[at, lanes]
                f3 = p_ref[at, lanes]
                direction = jnp.zeros_like(f3)
                for n in range(NEURONS):
                    inner = (
                        (g[3 * n] * by_g) * f1
                        + (g[3 * n + 1] * by_m) * f2
                        + g[3 * n + 2] * f3
                        + g[3 * NEURONS + n]
                    )
                    direction = direction + g[4 * NEURONS + n] * jnp.maximum(inner, 0.0)
                fresh = f3 - rate * direction
                if last is None:
                    if k == 1:
                        fresh = jnp.where(column < classes, fresh, 0.0)
                    refs[7][at, lanes] = fresh
                    refs[8 + k][at, :] = fresh.astype(BF16)
                elif k == 0:
                    outs[0][0, at, :] = fresh
                    outs[2][0, at, :] = f2
                else:
                    outs[1][0, at, :] = fresh[:, :classes]
                    outs[3][0, at, :] = f2[:, :classes]

    def final_kernel(*refs):
        nonlocal outs
        packed_ref, loss_ref = refs[7:9]
        outs = refs[9:]
        kernel(*refs[:7])
        s_ref = refs[0]
        total = s_ref[0]
        for i in range(1, members):
            total = total + s_ref[i]
        total = jnp.sum(total, axis=1, keepdims=True)
        earlier = jnp.sum(loss_ref[...], axis=(0, 1), keepdims=True)
        own = total[8:9, 0:1] / batch_total
        tasks = packed_ref.shape[0]
        scores = [total[9 + t : 10 + t, 0:1] / batch_total / steps for t in range(tasks)]
        center = scores[0]
        for score in scores[1:]:
            center = center + score
        center = center / tasks
        rows_out = outs[4].shape[0]
        meta = jnp.zeros(outs[4].shape, F32)
        for t, score in enumerate(scores):
            meta = meta + (score - center) * packed_ref[t, :rows_out, :]
        outs[4][...] = meta / (SIGMA * tasks)
        spot = lax.broadcasted_iota(jnp.int32, (1, steps), 1)
        outs[5][...] = jnp.where(spot == 0, earlier, own)

    def first_kernel(*refs):
        kernel(*refs)
        total = refs[0][0]
        for i in range(1, members):
            total = total + refs[0][i]
        own = jnp.sum(total[8:9, :], axis=1, keepdims=True) / batch_total
        place = lax.broadcasted_iota(jnp.int32, (8, 128), 0) + lax.broadcasted_iota(jnp.int32, (8, 128), 1)
        refs[10][...] = jnp.where(place == 0, jnp.broadcast_to(own, (8, 128)), 0.0)

    outs = None
    batch_total = counts[2]
    ins = [sums, theta, hyper_in, hyper_out, gradient, moment, tensor]
    if last is None:
        shapes = [shape_of((rows, both))] + [shape_of((rows, width), BF16)] * 2 + [shape_of((8, 128))]
        return call(first_kernel, ins, shapes)
    ins = ins + list(last)
    shapes = [
        shape_of((1, rows, width)),
        shape_of((1, rows, classes)),
        shape_of((1, rows, width)),
        shape_of((1, rows, classes)),
        shape_of((last[0].shape[1] - 8, last[0].shape[2])),
        shape_of((1, steps)),
    ]
    return call(final_kernel, ins, shapes)


def on_device(
    inputs, labels, w_hidden, w_out, mom_hidden, mom_out, signs, perturb, hyper_in, hyper_mid, hyper_out
):
    members = lax.axis_size(AXES)
    tasks = lax.axis_size("task")
    steps, batch, _ = inputs.shape[1:]
    rows, width = w_hidden.shape[1:]
    classes = w_out.shape[2]
    counts = (float(rows * members * width), float(rows * members * classes), float(batch * members))
    label_columns = labels.reshape(steps, batch, 1)
    hyper_out = jnp.pad(hyper_out, ((0, 0), (0, 128 - hyper_out.shape[1])))

    place = jnp.stack([lax.axis_index(axis) for axis in AXES]).astype(jnp.int32)
    send_a, send_b, signed = prepare(w_hidden, w_out, signs, perturb, hyper_mid)
    local_losses = []
    losses = []
    for step in range(steps):
        all_a, all_b, came = gathered(place, send_a, send_b)
        if step == 0:
            tensor, moment = side_by_side(w_hidden, w_out, mom_hidden, mom_out, came)
            theta = joined_theta(place, all_a, all_b, width, hyper_mid.shape[0])
        first, second, loss = forward_backward(place, inputs, label_columns, all_a, all_b, step, classes)
        local_losses.append(loss)
        is_last = step == steps - 1
        others = []
        if is_last:
            packed = packed_copies(signed, local_losses, tasks)
            others = [lax.all_to_all(packed, "task", split_axis=0, concat_axis=0, tiled=True)]
        parts = scattered(place, first, second, others)
        gradient, moment, sums = reduce_gradient(parts, moment, tensor, loss, others, members)
        sums = lax.all_to_all(sums, AXES, split_axis=0, concat_axis=0, tiled=True)
        last = (others[0], losses[0]) if is_last else None
        results = learned_update(
            sums, theta, hyper_in, hyper_out, gradient, moment, tensor, counts, step, steps, members, classes, last
        )
        if not is_last:
            tensor, send_a, send_b, loss_tile = results
            losses.append(loss_tile)
    new_hidden, new_out, new_mom_hidden, new_mom_out, meta_grad, loss_row = results
    return new_hidden, new_out, new_mom_hidden, new_mom_out, loss_row, meta_grad


def solution(mesh):
    split = Mesh(mesh.devices.reshape(mesh.shape["task"], RING, RING), ("task", *AXES))
    return jax.shard_map(
        on_device,
        mesh=split,
        in_specs=(
            P("task", None, AXES, None),
            P("task", None, AXES),
            P("task", AXES, None),
            P("task", AXES, None),
            P("task", AXES, None),
            P("task", AXES, None),
            P("task"),
            P("task", AXES, None),
            P(),
            P(AXES, None),
            P(),
        ),
        out_specs=(
            P("task", AXES, None),
            P("task", AXES, None),
            P("task", AXES, None),
            P("task", AXES, None),
            P("task", None),
            P(AXES, None),
        ),
        check_vma=False,
    )
```

```python
import jax
import jax.numpy as jnp
from jax import lax
from jax.experimental import pallas as pl
from jax.experimental.pallas import tpu as pltpu
from jax.sharding import Mesh
from jax.sharding import PartitionSpec as P

BETA = 0.8
FLOOR = 0.001
SIGMA = 0.01
LR_BASE = 0.03
NEURONS = 4
RING = 4
LINES = 24
AXES = ("dp_0", "dp_1")
HIGH = lax.Precision.HIGHEST
BY_ROWS = (((0,), (0,)), ((), ()))
BY_COLUMNS = (((1,), (1,)), ((), ()))
F32 = jnp.float32
BF16 = jnp.bfloat16


VMEM = pl.BlockSpec(memory_space=pltpu.VMEM)
HBM = pl.BlockSpec(memory_space=pltpu.HBM)
SMEM = pl.BlockSpec(memory_space=pltpu.SMEM)


def call(kernel, ins, outs, scratch=(), spaces=None, out_spaces=None, limit=12):
    return pl.pallas_call(
        kernel,
        in_specs=spaces or [VMEM] * len(ins),
        out_specs=out_spaces or [VMEM] * len(outs),
        out_shape=outs,
        scratch_shapes=list(scratch),
        compiler_params=pltpu.CompilerParams(vmem_limit_bytes=limit * 1024 * 1024),
    )(*ins)


def places():
    return [lax.axis_index(axis) for axis in AXES]


def shape_of(shape, dtype=F32):
    return jax.ShapeDtypeStruct(shape, dtype)


def fetch(pairs, sems):
    copies = [pltpu.make_async_copy(src, dst, sems.at[i]) for i, (src, dst) in enumerate(pairs)]
    for copy in copies:
        copy.start()
    return copies


def prepare(w_hidden, w_out, signs, perturb, hyper_mid):
    rows, width = w_hidden.shape[1:]
    classes = w_out.shape[2]
    trows, hyp = hyper_mid.shape
    half = hyp // 2

    def kernel(sign_ref, wh_any, wo_any, noise_any, mid_any, send_a, send_b, signed, wh, wo, noise, mid, sems):
        copies = fetch(((wh_any, wh), (wo_any, wo), (noise_any, noise), (mid_any, mid)), sems)
        copies[0].wait()
        send_a[:, :width] = wh[0].astype(BF16)
        copies[1].wait()
        pad = jnp.zeros((rows, width - classes), F32)
        send_b[:, :width] = jnp.concatenate([wo[0], pad], axis=1).astype(BF16)
        copies[2].wait()
        copies[3].wait()
        sign = sign_ref[0].astype(F32)
        signed[...] = sign * noise[0]
        theta = mid[...] + SIGMA * sign * noise[0]
        high = theta.astype(BF16)
        low = (theta - high.astype(F32)).astype(BF16)
        for ref, extra in ((send_a, high), (send_b, low)):
            ref[:trows, width:] = extra[:, :half]
            ref[trows:, width:] = extra[:, half:]

    outs = [
        shape_of((rows, width + half), BF16),
        shape_of((rows, width + half), BF16),
        shape_of((trows, hyp)),
    ]
    ins = (signs, w_hidden, w_out, perturb, hyper_mid)
    scratch = [pltpu.VMEM(a.shape, F32) for a in ins[1:]] + [pltpu.SemaphoreType.DMA((4,))]
    return call(kernel, ins, outs, scratch, [SMEM] + [HBM] * 4)


def side_by_side(w_hidden, w_out, mom_hidden, mom_out, after):
    rows, width = w_hidden.shape[1:]
    classes = w_out.shape[2]

    def kernel(wh_any, wo_any, mh_any, mo_any, _, tensor_any, moment_any, wh, wo, mh, mo, tensor, moment, sems):
        pairs = ((wh_any, wh), (wo_any, wo), (mh_any, mh), (mo_any, mo))
        for copy in fetch(pairs, sems):
            copy.wait()
        pad = jnp.zeros((rows, width - classes), F32)
        tensor[:, :width] = wh[0]
        tensor[:, width:] = jnp.concatenate([wo[0], pad], axis=1)
        moment[:, :width] = mh[0]
        moment[:, width:] = jnp.concatenate([mo[0], pad], axis=1)
        for copy in fetch(((tensor, tensor_any), (moment, moment_any)), sems):
            copy.wait()

    ins = (w_hidden, w_out, mom_hidden, mom_out, after)
    both = (rows, 2 * width)
    scratch = [pltpu.VMEM(a.shape, F32) for a in ins[:4]] + [pltpu.VMEM(both, F32)] * 2
    scratch = scratch + [pltpu.SemaphoreType.DMA((4,))]
    outs = [pltpu.HBM(both, F32)] * 2
    return call(kernel, ins, outs, scratch, [HBM] * 4 + [VMEM], [HBM] * 2)


def packed_with(signed, losses):
    trows, hyp = signed.shape

    def kernel(*refs):
        out = refs[-1]
        total = refs[1][...]
        for ref in refs[2:-1]:
            total = total + ref[...]
        out[:trows, :] = refs[0][...]
        out[trows:, :128] = total
        out[trows:, 128:] = jnp.zeros((8, hyp - 128), F32)

    return call(kernel, (signed, *losses), [shape_of((trows + 8, hyp))])[0]


def turned(place, k):
    return lax.rem(place + (RING - k), RING)


def shifted_copies(first, first_axis, second, second_axis):
    got = {}
    for k in (1, 3, 2):
        pairs = [(i, (i + k) % RING) for i in range(RING)]
        got[0, k] = lax.ppermute(first[k], first_axis, pairs)
        got[1, k] = lax.ppermute(second[k], second_axis, pairs)
    return (
        [first[0]] + [got[0, k] for k in range(1, RING)],
        [second[0]] + [got[1, k] for k in range(1, RING)],
    )


def gathered(send_a, send_b):
    rows, width = send_a.shape
    from_a, from_b = shifted_copies([send_a] * RING, AXES[1], [send_b] * RING, AXES[0])

    def kernel(*refs):
        place = places()
        for k in range(RING):
            refs[8][turned(place[1], k)] = refs[k][...]
            refs[9][turned(place[0], k)] = refs[4 + k][...]

    four_a, four_b = call(kernel, (*from_a, *from_b), [shape_of((RING, rows, width), BF16)] * 2)
    all_a, all_b = shifted_copies([four_a] * RING, AXES[0], [four_b] * RING, AXES[1])
    return all_a, all_b, from_a[1]


def joined_theta(all_a, all_b, width, trows):
    half = all_a[0].shape[2] - width

    def kernel(*refs):
        out = refs[8]
        place = places()
        for k in range(RING):
            z = turned(place[0], k)
            for j in range(RING):
                out[z * RING + j, :, :half] = refs[k][j, :trows, width:].astype(F32)
                out[z * RING + j, :, half:] = refs[k][j, trows:, width:].astype(F32)
        for k in range(RING):
            y = turned(place[1], k)
            for j in range(RING):
                at = j * RING + y
                out[at, :, :half] = out[at, :, :half] + refs[4 + k][j, :trows, width:].astype(F32)
                out[at, :, half:] = out[at, :, half:] + refs[4 + k][j, trows:, width:].astype(F32)

    (theta,) = call(kernel, (*all_a, *all_b), [shape_of((RING * RING, trows, 2 * half))])
    return theta


def forward_backward(inputs, labels, all_a, all_b, step, classes):
    batch, width = inputs.shape[2:]
    rows = all_a[0].shape[1]
    slab = RING * rows
    scale = width**-0.5
    chunk = batch // 2

    def kernel(x_any, y_ref, *refs):
        a_refs, b_refs = refs[:4], refs[4:8]
        g1_refs, g2_refs, loss_ref = refs[8:12], refs[12:16], refs[16]
        x_ref, w1_ref, w2_ref, act_ref, err_ref, dpre_ref, g_ref, sem = refs[17:]
        load = pltpu.make_async_copy(x_any.at[0, step], x_ref, sem)
        load.start()
        place = places()
        answers = jnp.broadcast_to(y_ref[0, step : step + 1, :], (128, batch)).T[:, 0:1]
        def place_weights(j, _):
            for k in range(RING):
                at = turned(place[0], k) * slab + j * rows
                w1_ref[pl.ds(pl.multiple_of(at, rows), rows), :] = a_refs[k][j, :, :width]
                at = j * slab + turned(place[1], k) * rows
                w2_ref[pl.ds(pl.multiple_of(at, rows), rows), :] = b_refs[k][j, :, :width]

        lax.fori_loop(0, RING, place_weights, None)
        load.wait()
        loss = jnp.zeros((1, 1), F32)
        for c in range(batch // chunk):
            part = slice(c * chunk, (c + 1) * chunk)
            before = jnp.dot(x_ref[part, :], w1_ref[...], preferred_element_type=F32) * scale
            active = jnp.maximum(before, 0.0).astype(BF16)
            act_ref[part, :] = active
            logits = jnp.dot(active, w2_ref[...], preferred_element_type=F32) * scale
            column = lax.broadcasted_iota(jnp.int32, logits.shape, 1)
            logits = jnp.where(column < classes, logits, -1e30)
            shifted = logits - jnp.max(logits, axis=1, keepdims=True)
            powers = jnp.exp(shifted)
            total = jnp.sum(powers, axis=1, keepdims=True)
            hit = column == answers[part, :]
            own = jnp.sum(jnp.where(hit, shifted, 0.0), axis=1, keepdims=True)
            loss = loss + jnp.sum(jnp.log(total) - own, axis=0, keepdims=True)
            errors = (powers * (1.0 / total) - hit.astype(F32)).astype(BF16)
            err_ref[part, :] = errors
            back = lax.dot_general(errors, w2_ref[...], BY_COLUMNS, preferred_element_type=F32) * scale
            dpre_ref[part, :] = jnp.where(before > 0, back, 0.0).astype(BF16)
        g_ref[...] = lax.dot_general(
            act_ref[...], err_ref[...], BY_ROWS, preferred_element_type=F32
        ).astype(BF16)

        def cut_second(j, _):
            for k in range(RING):
                at = j * slab + lax.rem(place[1] + k, RING) * rows
                g2_refs[k][j] = g_ref[pl.ds(pl.multiple_of(at, rows), rows), :]

        lax.fori_loop(0, RING, cut_second, None)
        g_ref[...] = lax.dot_general(
            x_ref[...], dpre_ref[...], BY_ROWS, preferred_element_type=F32
        ).astype(BF16)

        def cut_first(j, _):
            for k in range(RING):
                at = lax.rem(place[0] + k, RING) * slab + j * rows
                g1_refs[k][j] = g_ref[pl.ds(pl.multiple_of(at, rows), rows), :]

        lax.fori_loop(0, RING, cut_first, None)
        spot = lax.broadcasted_iota(jnp.int32, (8, 128), 0) + lax.broadcasted_iota(jnp.int32, (8, 128), 1)
        loss_ref[...] = jnp.where(spot == 0, jnp.broadcast_to(loss, (8, 128)), 0.0)

    outs = [shape_of((RING, rows, width), BF16)] * 8 + [shape_of((8, 128))]
    scratch = [pltpu.VMEM((batch, width), BF16)] + [pltpu.VMEM((width, width), BF16)] * 2
    scratch = scratch + [pltpu.VMEM((batch, width), BF16)] * 3 + [pltpu.VMEM((width, width), BF16)]
    scratch = scratch + [pltpu.SemaphoreType.DMA]
    spaces = [HBM] + [VMEM] * 9
    results = call(kernel, (inputs, labels, *all_a, *all_b), outs, scratch, spaces, limit=32)
    return results[:4], results[4:8], results[8]


def scattered(first, second, after):
    rows, width = first[0].shape[1:]
    first, second = shifted_copies(first, AXES[0], second, AXES[1])

    def kernel(*refs):
        outs = refs[-8:]
        place = places()

        def block(b, _):
            lines = pl.ds(pl.multiple_of(b * 16, 16), 16)
            for axis, ins, own in ((1, refs[:4], outs[:4]), (0, refs[4:8], outs[4:])):
                for k in range(RING):
                    at = lax.rem(place[axis] + k, RING)
                    total = ins[0][at, lines, :].astype(F32)
                    for i in range(1, RING):
                        total = total + ins[i][at, lines, :].astype(F32)
                    own[k][lines, :] = total.astype(own[k].dtype)

        lax.fori_loop(0, rows // 16, block, None)

    outs = ([shape_of((rows, width))] + [shape_of((rows, width), BF16)] * 3) * 2
    parts = call(kernel, (*first, *second, *after), outs)
    return shifted_copies(parts[:4], AXES[1], parts[4:], AXES[0])


def reduce_gradient(parts, moment, tensor, loss, others, members):
    rows, both = moment.shape
    width = both // 2
    scale = width**-0.5
    block = 16

    def kernel(*refs):
        r_refs, refs = refs[:8], refs[8:]
        m_any, p_any, loss_ref = refs[:3]
        other_refs = refs[3 : 3 + len(others)]
        g_any, m_out_any, s_ref, m_ref, p_ref, g_ref, m_out, sems = refs[3 + len(others) :]
        for copy in fetch(((m_any, m_ref), (p_any, p_ref)), sems):
            copy.wait()
        totals = [jnp.zeros((8, 128), F32) for _ in range(8)]
        for b in range(rows // block):
            at = slice(b * block, (b + 1) * block)
            for half in range(2):
                for q in range(2):
                    lanes = slice(half * width + q * width // 2, half * width + (q + 1) * width // 2)
                    own = slice(q * width // 2, (q + 1) * width // 2)
                    g = r_refs[4 * half][at, own]
                    for i in range(1, RING):
                        g = g + r_refs[4 * half + i][at, own].astype(F32)
                    g = g * scale
                    p = p_ref[at, lanes]
                    m = BETA * m_ref[at, lanes] + (1.0 - BETA) * g
                    g_ref[at, lanes] = g
                    m_out[at, lanes] = m
                    for k, product in enumerate((g * g, m * m, p * p, g * m)):
                        part = product[:8] + product[8:]
                        for j in range(width // 256):
                            totals[4 * half + k] = totals[4 * half + k] + part[:, j * 128 : (j + 1) * 128]
        lines = [jnp.sum(t, axis=0, keepdims=True) for t in totals]
        lines.append(loss_ref[0:1, :])
        for ref in other_refs:
            lines.append(ref[ref.shape[0] - 8 : ref.shape[0] - 7, :128])
        while len(lines) < LINES:
            lines.append(jnp.zeros((1, 128), F32))
        tile = jnp.concatenate(lines, axis=0)
        copies = fetch(((g_ref, g_any), (m_out, m_out_any)), sems)
        for i in range(members):
            s_ref[i] = tile
        for copy in copies:
            copy.wait()

    ins = (*parts[0], *parts[1], moment, tensor, loss, *others)
    outs = [pltpu.HBM((rows, both), F32)] * 2 + [shape_of((members, LINES, 128))]
    scratch = [pltpu.VMEM((rows, both), F32)] * 4 + [pltpu.SemaphoreType.DMA((2,))]
    spaces = [VMEM] * 8 + [HBM] * 2 + [VMEM] * (1 + len(others))
    return call(kernel, ins, outs, scratch, spaces, [HBM, HBM, VMEM])


def learned_update(sums, theta, hyper_in, hyper_out, gradient, moment, tensor, counts, step, steps, members, classes, last):
    rows, both = gradient.shape
    width = both // 2
    hyp = hyper_in.shape[1]

    def kernel(*refs):
        s_ref, t_ref, in_ref, out_ref = refs[:4]
        g_ref, m_ref, p_ref, sems = scratch_refs
        loads = fetch(((refs[4], g_ref), (refs[5], m_ref), (refs[6], p_ref)), sems)
        total = s_ref[0]
        for i in range(1, members):
            total = total + s_ref[i]
        total = jnp.sum(total, axis=1, keepdims=True)
        means = []
        opening = []
        for k in range(2):
            a, b, c, e = (total[4 * k + j : 4 * k + j + 1, 0:1] / counts[k] for j in range(4))
            means.append((a, b))
            z = (
                jnp.log(FLOOR + a),
                jnp.log(FLOOR + b),
                jnp.log(1.0 + c),
                e / jnp.sqrt((FLOOR + a) * (FLOOR + b)),
            )
            line = in_ref[4:5, :] * ((step + 1.0) / steps) + in_ref[5:6, :] + in_ref[6 + k : 7 + k, :]
            for j in range(4):
                line = line + z[j] * in_ref[j : j + 1, :]
            opening.append(line)
        opening.append(jnp.zeros((6, hyp), F32))
        opening = jnp.tanh(jnp.concatenate(opening, axis=0))
        middle = jnp.tanh(
            jnp.dot(opening, t_ref[...].reshape(hyp, hyp), precision=HIGH, preferred_element_type=F32)
        )
        coeffs = lax.dot_general(
            middle, out_ref[...], BY_COLUMNS, precision=HIGH, preferred_element_type=F32
        )
        for load in loads:
            load.wait()
        column = lax.broadcasted_iota(jnp.int32, (1, width), 1)
        for k in range(2):
            g = [coeffs[k : k + 1, j : j + 1] for j in range(5 * NEURONS + 1)]
            by_g = 1.0 / jnp.sqrt(FLOOR + means[k][0])
            by_m = 1.0 / jnp.sqrt(FLOOR + means[k][1])
            rate = LR_BASE * jnp.exp(g[5 * NEURONS])
            lanes = slice(k * width, (k + 1) * width)
            for b in range(rows // 16):
                at = slice(b * 16, (b + 1) * 16)
                f1 = g_ref[at, lanes]
                f2 = m_ref[at, lanes]
                f3 = p_ref[at, lanes]
                direction = jnp.zeros_like(f3)
                for n in range(NEURONS):
                    inner = (
                        (g[3 * n] * by_g) * f1
                        + (g[3 * n + 1] * by_m) * f2
                        + g[3 * n + 2] * f3
                        + g[3 * NEURONS + n]
                    )
                    direction = direction + g[4 * NEURONS + n] * jnp.maximum(inner, 0.0)
                fresh = f3 - rate * direction
                if last is None:
                    if k == 1:
                        fresh = jnp.where(column < classes, fresh, 0.0)
                    p_ref[at, lanes] = fresh
                    refs[8 + k][at, :] = fresh.astype(BF16)
                elif k == 0:
                    outs[0][0, at, :] = fresh
                    outs[2][0, at, :] = f2
                else:
                    outs[1][0, at, :] = fresh[:, :classes]
                    outs[3][0, at, :] = f2[:, :classes]

    def final_kernel(*refs):
        nonlocal outs, scratch_refs
        scratch_refs = refs[-4:]
        packed_refs, loss_ref = refs[7:-11], refs[-11]
        outs = refs[-10:-4]
        kernel(*refs[:7])
        s_ref = refs[0]
        total = s_ref[0]
        for i in range(1, members):
            total = total + s_ref[i]
        total = jnp.sum(total, axis=1, keepdims=True)
        earlier = jnp.sum(loss_ref[...], axis=(0, 1), keepdims=True)
        own = total[8:9, 0:1] / batch_total
        tasks = len(packed_refs)
        scores = [(earlier + own) / steps]
        for t in range(1, tasks):
            scores.append(total[8 + t : 9 + t, 0:1] / batch_total / steps)
        center = scores[0]
        for score in scores[1:]:
            center = center + score
        center = center / tasks
        rows_out = outs[4].shape[0]
        meta = jnp.zeros(outs[4].shape, F32)
        for score, ref in zip(scores, packed_refs):
            meta = meta + (score - center) * ref[:rows_out, :]
        outs[4][...] = meta / (SIGMA * tasks)
        spot = lax.broadcasted_iota(jnp.int32, (1, steps), 1)
        outs[5][...] = jnp.where(spot == 0, earlier, own)

    def first_kernel(*refs):
        nonlocal scratch_refs
        scratch_refs = refs[-4:]
        kernel(*refs[:-4])
        store = fetch(((scratch_refs[2], refs[7]),), scratch_refs[3])
        total = refs[0][0]
        for i in range(1, members):
            total = total + refs[0][i]
        own = jnp.sum(total[8:9, :], axis=1, keepdims=True) / batch_total
        place = lax.broadcasted_iota(jnp.int32, (8, 128), 0) + lax.broadcasted_iota(jnp.int32, (8, 128), 1)
        refs[10][...] = jnp.where(place == 0, jnp.broadcast_to(own, (8, 128)), 0.0)
        store[0].wait()

    outs = None
    scratch_refs = None
    batch_total = counts[2]
    ins = [sums, theta, hyper_in, hyper_out, gradient, moment, tensor]
    scratch = [pltpu.VMEM((rows, both), F32)] * 3 + [pltpu.SemaphoreType.DMA((3,))]
    spaces = [VMEM] * 4 + [HBM] * 3
    if last is None:
        shapes = [pltpu.HBM((rows, both), F32)] + [shape_of((rows, width), BF16)] * 2 + [shape_of((8, 128))]
        return call(first_kernel, ins, shapes, scratch, spaces, [HBM, VMEM, VMEM, VMEM])
    ins = ins + list(last)
    shapes = [
        shape_of((1, rows, width)),
        shape_of((1, rows, classes)),
        shape_of((1, rows, width)),
        shape_of((1, rows, classes)),
        shape_of((last[0].shape[0] - 8, last[0].shape[1])),
        shape_of((1, steps)),
    ]
    return call(final_kernel, ins, shapes, scratch, spaces + [VMEM] * len(last))


def on_device(
    inputs, labels, w_hidden, w_out, mom_hidden, mom_out, signs, perturb, hyper_in, hyper_mid, hyper_out
):
    members = lax.axis_size(AXES)
    tasks = lax.axis_size("task")
    steps, batch, _ = inputs.shape[1:]
    rows, width = w_hidden.shape[1:]
    classes = w_out.shape[2]
    counts = (float(rows * members * width), float(rows * members * classes), float(batch * members))
    hyper_out = hyper_out.T

    send_a, send_b, signed = prepare(w_hidden, w_out, signs, perturb, hyper_mid)
    local_losses = []
    losses = []
    for step in range(steps):
        all_a, all_b, came = gathered(send_a, send_b)
        if step == 0:
            tensor, moment = side_by_side(w_hidden, w_out, mom_hidden, mom_out, came)
            theta = joined_theta(all_a, all_b, width, hyper_mid.shape[0])
        first, second, loss = forward_backward(inputs, labels, all_a, all_b, step, classes)
        local_losses.append(loss)
        is_last = step == steps - 1
        others = []
        if is_last:
            packed = packed_with(signed, local_losses)
            others = [
                lax.ppermute(packed, "task", [(i, (i + k) % tasks) for i in range(tasks)])
                for k in range(1, tasks)
            ]
        parts = scattered(first, second, others)
        gradient, moment, sums = reduce_gradient(parts, moment, tensor, loss, others, members)
        sums = lax.all_to_all(sums, AXES, split_axis=0, concat_axis=0, tiled=True)
        last = (packed, *others, losses[0]) if is_last else None
        results = learned_update(
            sums, theta, hyper_in, hyper_out, gradient, moment, tensor, counts, step, steps, members, classes, last
        )
        if not is_last:
            tensor, send_a, send_b, loss_tile = results
            losses.append(loss_tile)
    new_hidden, new_out, new_mom_hidden, new_mom_out, meta_grad, loss_row = results
    return new_hidden, new_out, new_mom_hidden, new_mom_out, loss_row, meta_grad


def solution(mesh):
    split = Mesh(mesh.devices.reshape(mesh.shape["task"], RING, RING), ("task", *AXES))
    return jax.shard_map(
        on_device,
        mesh=split,
        in_specs=(
            P("task", None, AXES, None),
            P("task", None, AXES),
            P("task", AXES, None),
            P("task", AXES, None),
            P("task", AXES, None),
            P("task", AXES, None),
            P("task"),
            P("task", AXES, None),
            P(),
            P(AXES, None),
            P(),
        ),
        out_specs=(
            P("task", AXES, None),
            P("task", AXES, None),
            P("task", AXES, None),
            P("task", AXES, None),
            P("task", None),
            P(AXES, None),
        ),
        check_vma=False,
    )
```

```python
import jax
import jax.numpy as jnp
from jax import lax
from jax.experimental import pallas as pl
from jax.experimental.pallas import tpu as pltpu
from jax.sharding import Mesh
from jax.sharding import PartitionSpec as P

BETA = 0.8
FLOOR = 0.001
SIGMA = 0.01
LR_BASE = 0.03
NEURONS = 4
RING = 4
STAGGER = 3200
AXES = ("dp_0", "dp_1")
HIGH = lax.Precision.HIGHEST
BY_ROWS = (((0,), (0,)), ((), ()))
BY_COLUMNS = (((1,), (1,)), ((), ()))
F32 = jnp.float32
BF16 = jnp.bfloat16


VMEM = pl.BlockSpec(memory_space=pltpu.VMEM)
HBM = pl.BlockSpec(memory_space=pltpu.HBM)
SMEM = pl.BlockSpec(memory_space=pltpu.SMEM)


def call(kernel, ins, outs, scratch=(), spaces=None, out_spaces=None, limit=12):
    if spaces:
        ins = [
            pltpu.with_memory_space_constraint(a, pltpu.HBM) if space is HBM else a
            for a, space in zip(ins, spaces)
        ]
    return pl.pallas_call(
        kernel,
        in_specs=spaces or [VMEM] * len(ins),
        out_specs=out_spaces or [VMEM] * len(outs),
        out_shape=outs,
        scratch_shapes=list(scratch),
        compiler_params=pltpu.CompilerParams(vmem_limit_bytes=limit * 1024 * 1024),
    )(*ins)


def places():
    return [lax.axis_index(axis) for axis in AXES]


def shape_of(shape, dtype=F32):
    return jax.ShapeDtypeStruct(shape, dtype)


def fetch(pairs, sems):
    copies = [pltpu.make_async_copy(src, dst, sems.at[i]) for i, (src, dst) in enumerate(pairs)]
    for copy in copies:
        copy.start()
    return copies


def prepare(w_hidden, w_out, signs, perturb, hyper_mid):
    rows, width = w_hidden.shape[1:]
    classes = w_out.shape[2]
    trows, hyp = hyper_mid.shape
    half = hyp // 2

    def kernel(sign_ref, wh_any, wo_any, noise_any, mid_any, send_a, send_b, signed, wh, wo, noise, mid, wait_ref, sems):
        copies = fetch(((wh_any, wh), (wo_any, wo), (noise_any, noise), (mid_any, mid)), sems)
        turns = lax.rem(lax.axis_index("task"), 2) * STAGGER

        def turn(_, value):
            return value * 0.999 + 0.001

        wait_ref[...] = lax.fori_loop(0, turns, turn, jnp.ones((8, 128), F32))
        copies[0].wait()
        send_a[:, :width] = wh[0].astype(BF16)
        copies[1].wait()
        pad = jnp.zeros((rows, width - classes), F32)
        send_b[:, :width] = jnp.concatenate([wo[0], pad], axis=1).astype(BF16)
        copies[2].wait()
        copies[3].wait()
        sign = sign_ref[0].astype(F32)
        signed[...] = sign * noise[0]
        theta = mid[...] + SIGMA * sign * noise[0]
        high = theta.astype(BF16)
        low = (theta - high.astype(F32)).astype(BF16)
        for ref, extra in ((send_a, high), (send_b, low)):
            ref[:trows, width:] = extra[:, :half]
            ref[trows:, width:] = extra[:, half:]

    outs = [
        shape_of((rows, width + half), BF16),
        shape_of((rows, width + half), BF16),
        shape_of((trows, hyp)),
    ]
    ins = (signs, w_hidden, w_out, perturb, hyper_mid)
    scratch = [pltpu.VMEM(a.shape, F32) for a in ins[1:]]
    scratch = scratch + [pltpu.VMEM((8, 128), F32), pltpu.SemaphoreType.DMA((4,))]
    return call(kernel, ins, outs, scratch, [SMEM] + [HBM] * 4)


def side_by_side(w_hidden, w_out, mom_hidden, mom_out, after):
    rows, width = w_hidden.shape[1:]
    classes = w_out.shape[2]

    def kernel(wh_any, wo_any, mh_any, mo_any, _, tensor_any, moment_any, wh, wo, mh, mo, tensor, moment, sems):
        pairs = ((wh_any, wh), (wo_any, wo), (mh_any, mh), (mo_any, mo))
        for copy in fetch(pairs, sems):
            copy.wait()
        pad = jnp.zeros((rows, width - classes), F32)
        tensor[:, :width] = wh[0]
        tensor[:, width:] = jnp.concatenate([wo[0], pad], axis=1)
        moment[:, :width] = mh[0]
        moment[:, width:] = jnp.concatenate([mo[0], pad], axis=1)
        for copy in fetch(((tensor, tensor_any), (moment, moment_any)), sems):
            copy.wait()

    ins = (w_hidden, w_out, mom_hidden, mom_out, after)
    both = (rows, 2 * width)
    scratch = [pltpu.VMEM(a.shape, F32) for a in ins[:4]] + [pltpu.VMEM(both, F32)] * 2
    scratch = scratch + [pltpu.SemaphoreType.DMA((4,))]
    outs = [pltpu.HBM(both, F32)] * 2
    return call(kernel, ins, outs, scratch, [HBM] * 4 + [VMEM], [HBM] * 2)


def packed_with(signed, losses):
    trows, hyp = signed.shape

    def kernel(*refs):
        out = refs[-1]
        total = refs[1][...]
        for ref in refs[2:-1]:
            total = total + ref[...]
        out[:trows, :] = refs[0][...]
        out[trows:, :128] = total
        out[trows:, 128:] = jnp.zeros((8, hyp - 128), F32)

    return call(kernel, (signed, *losses), [shape_of((trows + 8, hyp))])[0]


def turned(place, k):
    return lax.rem(place + (RING - k), RING)


def shifted_copies(first, first_axis, second, second_axis):
    got = {}
    for k in (1, 3, 2):
        pairs = [(i, (i + k) % RING) for i in range(RING)]
        got[0, k] = lax.ppermute(first[k], first_axis, pairs)
        got[1, k] = lax.ppermute(second[k], second_axis, pairs)
    return (
        [first[0]] + [got[0, k] for k in range(1, RING)],
        [second[0]] + [got[1, k] for k in range(1, RING)],
    )


def gathered(send_a, send_b):
    rows, width = send_a.shape
    from_a, from_b = shifted_copies([send_a] * RING, AXES[1], [send_b] * RING, AXES[0])

    def kernel(*refs):
        place = places()
        for k in range(RING):
            refs[8][turned(place[1], k)] = refs[k][...]
            refs[9][turned(place[0], k)] = refs[4 + k][...]

    four_a, four_b = call(kernel, (*from_a, *from_b), [shape_of((RING, rows, width), BF16)] * 2)
    all_a, all_b = shifted_copies([four_a] * RING, AXES[0], [four_b] * RING, AXES[1])
    return all_a, all_b, from_a[1]


def joined_theta(all_a, all_b, width, trows):
    half = all_a[0].shape[2] - width

    def kernel(*refs):
        out = refs[8]
        place = places()
        for k in range(RING):
            z = turned(place[0], k)
            for j in range(RING):
                out[z * RING + j, :, :half] = refs[k][j, :trows, width:].astype(F32)
                out[z * RING + j, :, half:] = refs[k][j, trows:, width:].astype(F32)
        for k in range(RING):
            y = turned(place[1], k)
            for j in range(RING):
                at = j * RING + y
                out[at, :, :half] = out[at, :, :half] + refs[4 + k][j, :trows, width:].astype(F32)
                out[at, :, half:] = out[at, :, half:] + refs[4 + k][j, trows:, width:].astype(F32)

    (theta,) = call(kernel, (*all_a, *all_b), [shape_of((RING * RING, trows, 2 * half))])
    return theta


def forward_backward(inputs, labels, all_a, all_b, step, classes):
    batch, width = inputs.shape[2:]
    rows = all_a[0].shape[1]
    slab = RING * rows
    scale = width**-0.5
    chunk = batch // 2

    def kernel(x_any, y_ref, *refs):
        a_refs, b_refs = refs[:4], refs[4:8]
        g1_refs, g2_refs, loss_ref = refs[8:12], refs[12:16], refs[16]
        x_ref, w1_ref, w2_ref, act_ref, err_ref, dpre_ref, g_ref, sem = refs[17:]
        load = pltpu.make_async_copy(x_any.at[0, step], x_ref, sem)
        load.start()
        place = places()
        answers = jnp.broadcast_to(y_ref[0, step : step + 1, :], (128, batch)).T[:, 0:1]
        def place_weights(j, _):
            for k in range(RING):
                at = turned(place[0], k) * slab + j * rows
                w1_ref[pl.ds(pl.multiple_of(at, rows), rows), :] = a_refs[k][j, :, :width]
                at = j * slab + turned(place[1], k) * rows
                w2_ref[pl.ds(pl.multiple_of(at, rows), rows), :] = b_refs[k][j, :, :width]

        lax.fori_loop(0, RING, place_weights, None)
        load.wait()
        loss = jnp.zeros((1, 1), F32)
        for c in range(batch // chunk):
            part = slice(c * chunk, (c + 1) * chunk)
            before = jnp.dot(x_ref[part, :], w1_ref[...], preferred_element_type=F32) * scale
            active = jnp.maximum(before, 0.0).astype(BF16)
            act_ref[part, :] = active
            logits = jnp.dot(active, w2_ref[...], preferred_element_type=F32) * scale
            column = lax.broadcasted_iota(jnp.int32, logits.shape, 1)
            logits = jnp.where(column < classes, logits, -1e30)
            shifted = logits - jnp.max(logits, axis=1, keepdims=True)
            powers = jnp.exp(shifted)
            total = jnp.sum(powers, axis=1, keepdims=True)
            hit = column == answers[part, :]
            own = jnp.sum(jnp.where(hit, shifted, 0.0), axis=1, keepdims=True)
            loss = loss + jnp.sum(jnp.log(total) - own, axis=0, keepdims=True)
            errors = (powers * (1.0 / total) - hit.astype(F32)).astype(BF16)
            err_ref[part, :] = errors
            back = lax.dot_general(errors, w2_ref[...], BY_COLUMNS, preferred_element_type=F32) * scale
            dpre_ref[part, :] = jnp.where(before > 0, back, 0.0).astype(BF16)
        g_ref[...] = lax.dot_general(
            act_ref[...], err_ref[...], BY_ROWS, preferred_element_type=F32
        ).astype(BF16)

        def cut_second(j, _):
            for k in range(RING):
                at = j * slab + lax.rem(place[1] + k, RING) * rows
                g2_refs[k][j] = g_ref[pl.ds(pl.multiple_of(at, rows), rows), :]

        lax.fori_loop(0, RING, cut_second, None)
        g_ref[...] = lax.dot_general(
            x_ref[...], dpre_ref[...], BY_ROWS, preferred_element_type=F32
        ).astype(BF16)

        def cut_first(j, _):
            for k in range(RING):
                at = lax.rem(place[0] + k, RING) * slab + j * rows
                g1_refs[k][j] = g_ref[pl.ds(pl.multiple_of(at, rows), rows), :]

        lax.fori_loop(0, RING, cut_first, None)
        spot = lax.broadcasted_iota(jnp.int32, (8, 128), 0) + lax.broadcasted_iota(jnp.int32, (8, 128), 1)
        loss_ref[...] = jnp.where(spot == 0, jnp.broadcast_to(loss, (8, 128)), 0.0)

    outs = [shape_of((RING, rows, width), BF16)] * 8 + [shape_of((8, 128))]
    scratch = [pltpu.VMEM((batch, width), BF16)] + [pltpu.VMEM((width, width), BF16)] * 2
    scratch = scratch + [pltpu.VMEM((batch, width), BF16)] * 3 + [pltpu.VMEM((width, width), BF16)]
    scratch = scratch + [pltpu.SemaphoreType.DMA]
    spaces = [HBM] + [VMEM] * 9
    results = call(kernel, (inputs, labels, *all_a, *all_b), outs, scratch, spaces, limit=32)
    return results[:4], results[4:8], results[8]


def scattered(first, second, after):
    rows, width = first[0].shape[1:]
    first, second = shifted_copies(first, AXES[0], second, AXES[1])

    def kernel(*refs):
        outs = refs[-8:]
        place = places()

        def block(b, _):
            lines = pl.ds(pl.multiple_of(b * 16, 16), 16)
            for axis, ins, own in ((1, refs[:4], outs[:4]), (0, refs[4:8], outs[4:])):
                for k in range(RING):
                    at = lax.rem(place[axis] + k, RING)
                    total = ins[0][at, lines, :].astype(F32)
                    for i in range(1, RING):
                        total = total + ins[i][at, lines, :].astype(F32)
                    own[k][lines, :] = total.astype(own[k].dtype)

        lax.fori_loop(0, rows // 16, block, None)

    outs = ([shape_of((rows, width))] + [shape_of((rows, width), BF16)] * 3) * 2
    parts = call(kernel, (*first, *second, *after), outs)
    return shifted_copies(parts[:4], AXES[1], parts[4:], AXES[0])


def reduce_gradient(parts, moment, tensor, loss, others, members):
    rows, both = moment.shape
    width = both // 2
    scale = width**-0.5
    block = 16

    def kernel(*refs):
        r_refs, refs = refs[:8], refs[8:]
        m_any, p_any, loss_ref = refs[:3]
        other_refs = refs[3 : 3 + len(others)]
        g_any, m_out_any, s_ref, m_ref, p_ref, g_ref, m_out, sems = refs[3 + len(others) :]
        for copy in fetch(((m_any, m_ref), (p_any, p_ref)), sems):
            copy.wait()
        totals = [jnp.zeros((8, 128), F32) for _ in range(8)]
        for b in range(rows // block):
            at = slice(b * block, (b + 1) * block)
            for half in range(2):
                for q in range(2):
                    lanes = slice(half * width + q * width // 2, half * width + (q + 1) * width // 2)
                    own = slice(q * width // 2, (q + 1) * width // 2)
                    g = r_refs[4 * half][at, own]
                    for i in range(1, RING):
                        g = g + r_refs[4 * half + i][at, own].astype(F32)
                    g = g * scale
                    p = p_ref[at, lanes]
                    m = BETA * m_ref[at, lanes] + (1.0 - BETA) * g
                    g_ref[at, lanes] = g
                    m_out[at, lanes] = m
                    for k, product in enumerate((g * g, m * m, p * p, g * m)):
                        part = product[:8] + product[8:]
                        for j in range(width // 256):
                            totals[4 * half + k] = totals[4 * half + k] + part[:, j * 128 : (j + 1) * 128]
        lines = totals + [loss_ref[...]] + [ref[ref.shape[0] - 8 :, :128] for ref in other_refs]
        spot = lax.broadcasted_iota(jnp.int32, (8, 128), 1)
        tile = jnp.zeros((8, 128), F32)
        for k, line in enumerate(lines):
            column = jnp.sum(line, axis=1, keepdims=True)
            tile = jnp.where(spot == k, column, tile)
        copies = fetch(((g_ref, g_any), (m_out, m_out_any)), sems)
        for i in range(members):
            s_ref[i] = tile
        for copy in copies:
            copy.wait()

    ins = (*parts[0], *parts[1], moment, tensor, loss, *others)
    outs = [pltpu.HBM((rows, both), F32)] * 2 + [shape_of((members, 8, 128))]
    scratch = [pltpu.VMEM((rows, both), F32)] * 4 + [pltpu.SemaphoreType.DMA((2,))]
    spaces = [VMEM] * 8 + [HBM] * 2 + [VMEM] * (1 + len(others))
    return call(kernel, ins, outs, scratch, spaces, [HBM, HBM, VMEM])


def learned_update(sums, theta, hyper_in, hyper_out, gradient, moment, tensor, counts, step, steps, members, classes, last):
    rows, both = gradient.shape
    width = both // 2
    hyp = hyper_in.shape[1]

    def kernel(*refs):
        s_ref, t_ref, in_ref, out_ref = refs[:4]
        g_ref, m_ref, p_ref, sems = scratch_refs
        loads = fetch(((refs[4], g_ref), (refs[5], m_ref), (refs[6], p_ref)), sems)
        total = s_ref[0]
        for i in range(1, members):
            total = total + s_ref[i]
        total = jnp.sum(total, axis=0, keepdims=True)
        means = []
        opening = []
        for k in range(2):
            a, b, c, e = (total[:, 4 * k + j : 4 * k + j + 1] / counts[k] for j in range(4))
            means.append((a, b))
            z = (
                jnp.log(FLOOR + a),
                jnp.log(FLOOR + b),
                jnp.log(1.0 + c),
                e / jnp.sqrt((FLOOR + a) * (FLOOR + b)),
            )
            line = in_ref[4:5, :] * ((step + 1.0) / steps) + in_ref[5:6, :] + in_ref[6 + k : 7 + k, :]
            for j in range(4):
                line = line + z[j] * in_ref[j : j + 1, :]
            opening.append(line)
        opening.append(jnp.zeros((6, hyp), F32))
        opening = jnp.tanh(jnp.concatenate(opening, axis=0))
        middle = jnp.tanh(
            jnp.dot(opening, t_ref[...].reshape(hyp, hyp), precision=HIGH, preferred_element_type=F32)
        )
        coeffs = lax.dot_general(
            middle, out_ref[...], BY_COLUMNS, precision=HIGH, preferred_element_type=F32
        )
        for load in loads:
            load.wait()
        column = lax.broadcasted_iota(jnp.int32, (1, width), 1)
        for k in range(2):
            g = [coeffs[k : k + 1, j : j + 1] for j in range(5 * NEURONS + 1)]
            by_g = 1.0 / jnp.sqrt(FLOOR + means[k][0])
            by_m = 1.0 / jnp.sqrt(FLOOR + means[k][1])
            rate = LR_BASE * jnp.exp(g[5 * NEURONS])
            lanes = slice(k * width, (k + 1) * width)
            for b in range(rows // 16):
                at = slice(b * 16, (b + 1) * 16)
                f1 = g_ref[at, lanes]
                f2 = m_ref[at, lanes]
                f3 = p_ref[at, lanes]
                direction = jnp.zeros_like(f3)
                for n in range(NEURONS):
                    inner = (
                        (g[3 * n] * by_g) * f1
                        + (g[3 * n + 1] * by_m) * f2
                        + g[3 * n + 2] * f3
                        + g[3 * NEURONS + n]
                    )
                    direction = direction + g[4 * NEURONS + n] * jnp.maximum(inner, 0.0)
                fresh = f3 - rate * direction
                if last is None:
                    if k == 1:
                        fresh = jnp.where(column < classes, fresh, 0.0)
                    p_ref[at, lanes] = fresh
                    refs[8 + k][at, :] = fresh.astype(BF16)
                elif k == 0:
                    outs[0][0, at, :] = fresh
                    outs[2][0, at, :] = f2
                else:
                    outs[1][0, at, :] = fresh[:, :classes]
                    outs[3][0, at, :] = f2[:, :classes]

    def final_kernel(*refs):
        nonlocal outs, scratch_refs
        scratch_refs = refs[-4:]
        packed_refs, loss_ref = refs[7:-11], refs[-11]
        outs = refs[-10:-4]
        kernel(*refs[:7])
        s_ref = refs[0]
        total = s_ref[0]
        for i in range(1, members):
            total = total + s_ref[i]
        total = jnp.sum(total, axis=0, keepdims=True)
        earlier = jnp.sum(loss_ref[...], axis=(0, 1), keepdims=True)
        own = total[:, 8:9] / batch_total
        tasks = len(packed_refs)
        scores = [(earlier + own) / steps]
        for t in range(1, tasks):
            scores.append(total[:, 8 + t : 9 + t] / batch_total / steps)
        center = scores[0]
        for score in scores[1:]:
            center = center + score
        center = center / tasks
        rows_out = outs[4].shape[0]
        meta = jnp.zeros(outs[4].shape, F32)
        for score, ref in zip(scores, packed_refs):
            meta = meta + (score - center) * ref[:rows_out, :]
        outs[4][...] = meta / (SIGMA * tasks)
        spot = lax.broadcasted_iota(jnp.int32, (1, steps), 1)
        outs[5][...] = jnp.where(spot == 0, earlier, own)

    def first_kernel(*refs):
        nonlocal scratch_refs
        scratch_refs = refs[-4:]
        kernel(*refs[:-4])
        store = fetch(((scratch_refs[2], refs[7]),), scratch_refs[3])
        total = refs[0][0]
        for i in range(1, members):
            total = total + refs[0][i]
        own = jnp.sum(total[:, 8:9], axis=0, keepdims=True) / batch_total
        place = lax.broadcasted_iota(jnp.int32, (8, 128), 0) + lax.broadcasted_iota(jnp.int32, (8, 128), 1)
        refs[10][...] = jnp.where(place == 0, jnp.broadcast_to(own, (8, 128)), 0.0)
        store[0].wait()

    outs = None
    scratch_refs = None
    batch_total = counts[2]
    ins = [sums, theta, hyper_in, hyper_out, gradient, moment, tensor]
    scratch = [pltpu.VMEM((rows, both), F32)] * 3 + [pltpu.SemaphoreType.DMA((3,))]
    spaces = [VMEM] * 4 + [HBM] * 3
    if last is None:
        shapes = [pltpu.HBM((rows, both), F32)] + [shape_of((rows, width), BF16)] * 2 + [shape_of((8, 128))]
        return call(first_kernel, ins, shapes, scratch, spaces, [HBM, VMEM, VMEM, VMEM])
    ins = ins + list(last)
    shapes = [
        shape_of((1, rows, width)),
        shape_of((1, rows, classes)),
        shape_of((1, rows, width)),
        shape_of((1, rows, classes)),
        shape_of((last[0].shape[0] - 8, last[0].shape[1])),
        shape_of((1, steps)),
    ]
    return call(final_kernel, ins, shapes, scratch, spaces + [VMEM] * len(last))


def on_device(
    inputs, labels, w_hidden, w_out, mom_hidden, mom_out, signs, perturb, hyper_in, hyper_mid, hyper_out
):
    members = lax.axis_size(AXES)
    tasks = lax.axis_size("task")
    steps, batch, _ = inputs.shape[1:]
    rows, width = w_hidden.shape[1:]
    classes = w_out.shape[2]
    counts = (float(rows * members * width), float(rows * members * classes), float(batch * members))
    hyper_out = hyper_out.T

    send_a, send_b, signed = prepare(w_hidden, w_out, signs, perturb, hyper_mid)
    local_losses = []
    losses = []
    for step in range(steps):
        all_a, all_b, came = gathered(send_a, send_b)
        if step == 0:
            tensor, moment = side_by_side(w_hidden, w_out, mom_hidden, mom_out, came)
            theta = joined_theta(all_a, all_b, width, hyper_mid.shape[0])
        first, second, loss = forward_backward(inputs, labels, all_a, all_b, step, classes)
        local_losses.append(loss)
        is_last = step == steps - 1
        others = []
        if is_last:
            packed = packed_with(signed, local_losses)
            others = [
                lax.ppermute(packed, "task", [(i, (i + k) % tasks) for i in range(tasks)])
                for k in range(1, tasks)
            ]
        parts = scattered(first, second, others)
        gradient, moment, sums = reduce_gradient(parts, moment, tensor, loss, others, members)
        sums = lax.all_to_all(sums, AXES, split_axis=0, concat_axis=0, tiled=True)
        last = (packed, *others, losses[0]) if is_last else None
        results = learned_update(
            sums, theta, hyper_in, hyper_out, gradient, moment, tensor, counts, step, steps, members, classes, last
        )
        if not is_last:
            tensor, send_a, send_b, loss_tile = results
            losses.append(loss_tile)
    new_hidden, new_out, new_mom_hidden, new_mom_out, meta_grad, loss_row = results
    return new_hidden, new_out, new_mom_hidden, new_mom_out, loss_row, meta_grad


def solution(mesh):
    split = Mesh(mesh.devices.reshape(mesh.shape["task"], RING, RING), ("task", *AXES))
    return jax.shard_map(
        on_device,
        mesh=split,
        in_specs=(
            P("task", None, AXES, None),
            P("task", None, AXES),
            P("task", AXES, None),
            P("task", AXES, None),
            P("task", AXES, None),
            P("task", AXES, None),
            P("task"),
            P("task", AXES, None),
            P(),
            P(AXES, None),
            P(),
        ),
        out_specs=(
            P("task", AXES, None),
            P("task", AXES, None),
            P("task", AXES, None),
            P("task", AXES, None),
            P("task", None),
            P(AXES, None),
        ),
        check_vma=False,
    )
```

```python
import jax
import jax.numpy as jnp
from jax import lax
from jax.experimental import pallas as pl
from jax.experimental.pallas import tpu as pltpu
from jax.sharding import Mesh
from jax.sharding import PartitionSpec as P

BETA = 0.8
FLOOR = 0.001
SIGMA = 0.01
LR_BASE = 0.03
NEURONS = 4
RING = 4
STAGGER = 3000
AXES = ("dp_0", "dp_1")
HIGH = lax.Precision.HIGHEST
BY_ROWS = (((0,), (0,)), ((), ()))
BY_COLUMNS = (((1,), (1,)), ((), ()))
F32 = jnp.float32
BF16 = jnp.bfloat16


VMEM = pl.BlockSpec(memory_space=pltpu.VMEM)
HBM = pl.BlockSpec(memory_space=pltpu.HBM)
SMEM = pl.BlockSpec(memory_space=pltpu.SMEM)


def call(kernel, ins, outs, scratch=(), spaces=None, out_spaces=None, limit=12):
    if spaces:
        ins = [
            pltpu.with_memory_space_constraint(a, pltpu.HBM) if space is HBM else a
            for a, space in zip(ins, spaces)
        ]
    return pl.pallas_call(
        kernel,
        in_specs=spaces or [VMEM] * len(ins),
        out_specs=out_spaces or [VMEM] * len(outs),
        out_shape=outs,
        scratch_shapes=list(scratch),
        compiler_params=pltpu.CompilerParams(vmem_limit_bytes=limit * 1024 * 1024),
    )(*ins)


def places():
    return [lax.axis_index(axis) for axis in AXES]


def shape_of(shape, dtype=F32):
    return jax.ShapeDtypeStruct(shape, dtype)


def fetch(pairs, sems):
    copies = [pltpu.make_async_copy(src, dst, sems.at[i]) for i, (src, dst) in enumerate(pairs)]
    for copy in copies:
        copy.start()
    return copies


def prepare(w_hidden, w_out, signs, perturb, hyper_mid):
    rows, width = w_hidden.shape[1:]
    classes = w_out.shape[2]
    trows, hyp = hyper_mid.shape
    half = hyp // 2

    def kernel(sign_ref, wh_any, wo_any, noise_any, mid_any, send_a, send_b, signed, wh, wo, noise, mid, wait_ref, sems):
        copies = fetch(((wh_any, wh), (wo_any, wo), (noise_any, noise), (mid_any, mid)), sems)
        turns = lax.rem(lax.axis_index("task"), 2) * STAGGER

        def turn(_, value):
            return value * 0.999 + 0.001

        wait_ref[...] = lax.fori_loop(0, turns, turn, jnp.ones((8, 128), F32))
        copies[0].wait()
        send_a[:, :width] = wh[0].astype(BF16)
        copies[1].wait()
        pad = jnp.zeros((rows, width - classes), F32)
        send_b[:, :width] = jnp.concatenate([wo[0], pad], axis=1).astype(BF16)
        copies[2].wait()
        copies[3].wait()
        sign = sign_ref[0].astype(F32)
        signed[...] = sign * noise[0]
        theta = mid[...] + SIGMA * sign * noise[0]
        high = theta.astype(BF16)
        low = (theta - high.astype(F32)).astype(BF16)
        for ref, extra in ((send_a, high), (send_b, low)):
            ref[:trows, width:] = extra[:, :half]
            ref[trows:, width:] = extra[:, half:]

    outs = [
        shape_of((rows, width + half), BF16),
        shape_of((rows, width + half), BF16),
        shape_of((trows, hyp)),
    ]
    ins = (signs, w_hidden, w_out, perturb, hyper_mid)
    scratch = [pltpu.VMEM(a.shape, F32) for a in ins[1:]]
    scratch = scratch + [pltpu.VMEM((8, 128), F32), pltpu.SemaphoreType.DMA((4,))]
    return call(kernel, ins, outs, scratch, [SMEM] + [HBM] * 4)


def side_by_side(w_hidden, w_out, mom_hidden, mom_out, after):
    rows, width = w_hidden.shape[1:]
    classes = w_out.shape[2]

    def kernel(wh_any, wo_any, mh_any, mo_any, _, tensor_any, moment_any, wh, wo, mh, mo, tensor, moment, sems):
        pairs = ((wh_any, wh), (wo_any, wo), (mh_any, mh), (mo_any, mo))
        for copy in fetch(pairs, sems):
            copy.wait()
        pad = jnp.zeros((rows, width - classes), F32)
        tensor[:, :width] = wh[0]
        tensor[:, width:] = jnp.concatenate([wo[0], pad], axis=1)
        moment[:, :width] = mh[0]
        moment[:, width:] = jnp.concatenate([mo[0], pad], axis=1)
        for copy in fetch(((tensor, tensor_any), (moment, moment_any)), sems):
            copy.wait()

    ins = (w_hidden, w_out, mom_hidden, mom_out, after)
    both = (rows, 2 * width)
    scratch = [pltpu.VMEM(a.shape, F32) for a in ins[:4]] + [pltpu.VMEM(both, F32)] * 2
    scratch = scratch + [pltpu.SemaphoreType.DMA((4,))]
    outs = [pltpu.HBM(both, F32)] * 2
    return call(kernel, ins, outs, scratch, [HBM] * 4 + [VMEM], [HBM] * 2)


def packed_with(signed, losses):
    trows, hyp = signed.shape

    def kernel(*refs):
        out = refs[-1]
        total = refs[1][...]
        for ref in refs[2:-1]:
            total = total + ref[...]
        out[:trows, :] = refs[0][...]
        out[trows:, :128] = total
        out[trows:, 128:] = jnp.zeros((8, hyp - 128), F32)

    return call(kernel, (signed, *losses), [shape_of((trows + 8, hyp))])[0]


def turned(place, k):
    return lax.rem(place + (RING - k), RING)


def shifted_copies(first, first_axis, second, second_axis):
    got = {}
    for k in (1, 3, 2):
        pairs = [(i, (i + k) % RING) for i in range(RING)]
        got[0, k] = lax.ppermute(first[k], first_axis, pairs)
        got[1, k] = lax.ppermute(second[k], second_axis, pairs)
    return (
        [first[0]] + [got[0, k] for k in range(1, RING)],
        [second[0]] + [got[1, k] for k in range(1, RING)],
    )


def gathered(send_a, send_b):
    rows, width = send_a.shape
    from_a, from_b = shifted_copies([send_a] * RING, AXES[1], [send_b] * RING, AXES[0])

    def kernel(*refs):
        place = places()
        for k in range(RING):
            refs[8][turned(place[1], k)] = refs[k][...]
            refs[9][turned(place[0], k)] = refs[4 + k][...]

    four_a, four_b = call(kernel, (*from_a, *from_b), [shape_of((RING, rows, width), BF16)] * 2)
    all_a, all_b = shifted_copies([four_a] * RING, AXES[0], [four_b] * RING, AXES[1])
    return all_a, all_b, from_a[1]


def joined_theta(all_a, all_b, width, trows):
    half = all_a[0].shape[2] - width

    def kernel(*refs):
        out = refs[8]
        place = places()
        for k in range(RING):
            z = turned(place[0], k)
            for j in range(RING):
                out[z * RING + j, :, :half] = refs[k][j, :trows, width:].astype(F32)
                out[z * RING + j, :, half:] = refs[k][j, trows:, width:].astype(F32)
        for k in range(RING):
            y = turned(place[1], k)
            for j in range(RING):
                at = j * RING + y
                out[at, :, :half] = out[at, :, :half] + refs[4 + k][j, :trows, width:].astype(F32)
                out[at, :, half:] = out[at, :, half:] + refs[4 + k][j, trows:, width:].astype(F32)

    (theta,) = call(kernel, (*all_a, *all_b), [shape_of((RING * RING, trows, 2 * half))])
    return theta


def forward_backward(inputs, labels, all_a, all_b, step, classes):
    batch, width = inputs.shape[2:]
    rows = all_a[0].shape[1]
    slab = RING * rows
    scale = width**-0.5
    chunk = batch

    def kernel(x_any, y_ref, *refs):
        a_refs, b_refs = refs[:4], refs[4:8]
        g1_refs, g2_refs, loss_ref = refs[8:12], refs[12:16], refs[16]
        x_ref, w1_ref, w2_ref, act_ref, err_ref, dpre_ref, g_ref, sem = refs[17:]
        load = pltpu.make_async_copy(x_any.at[0, step], x_ref, sem)
        load.start()
        place = places()
        answers = jnp.broadcast_to(y_ref[0, step : step + 1, :], (128, batch)).T[:, 0:1]
        def place_weights(j, _):
            for k in range(RING):
                at = turned(place[0], k) * slab + j * rows
                w1_ref[pl.ds(pl.multiple_of(at, rows), rows), :] = a_refs[k][j, :, :width]
                at = j * slab + turned(place[1], k) * rows
                w2_ref[pl.ds(pl.multiple_of(at, rows), rows), :] = b_refs[k][j, :, :width]

        lax.fori_loop(0, RING, place_weights, None)
        load.wait()
        loss = jnp.zeros((1, 1), F32)
        for c in range(batch // chunk):
            part = slice(c * chunk, (c + 1) * chunk)
            before = jnp.dot(x_ref[part, :], w1_ref[...], preferred_element_type=F32) * scale
            active = jnp.maximum(before, 0.0).astype(BF16)
            act_ref[part, :] = active
            logits = jnp.dot(active, w2_ref[...], preferred_element_type=F32) * scale
            column = lax.broadcasted_iota(jnp.int32, logits.shape, 1)
            logits = jnp.where(column < classes, logits, -1e30)
            shifted = logits - jnp.max(logits, axis=1, keepdims=True)
            powers = jnp.exp(shifted)
            total = jnp.sum(powers, axis=1, keepdims=True)
            hit = column == answers[part, :]
            own = jnp.sum(jnp.where(hit, shifted, 0.0), axis=1, keepdims=True)
            loss = loss + jnp.sum(jnp.log(total) - own, axis=0, keepdims=True)
            errors = (powers * (1.0 / total) - hit.astype(F32)).astype(BF16)
            err_ref[part, :] = errors
            back = lax.dot_general(errors, w2_ref[...], BY_COLUMNS, preferred_element_type=F32) * scale
            dpre_ref[part, :] = jnp.where(before > 0, back, 0.0).astype(BF16)
        g_ref[...] = lax.dot_general(
            act_ref[...], err_ref[...], BY_ROWS, preferred_element_type=F32
        ).astype(BF16)

        def cut_second(j, _):
            for k in range(RING):
                at = j * slab + lax.rem(place[1] + k, RING) * rows
                g2_refs[k][j] = g_ref[pl.ds(pl.multiple_of(at, rows), rows), :]

        lax.fori_loop(0, RING, cut_second, None)
        g_ref[...] = lax.dot_general(
            x_ref[...], dpre_ref[...], BY_ROWS, preferred_element_type=F32
        ).astype(BF16)

        def cut_first(j, _):
            for k in range(RING):
                at = lax.rem(place[0] + k, RING) * slab + j * rows
                g1_refs[k][j] = g_ref[pl.ds(pl.multiple_of(at, rows), rows), :]

        lax.fori_loop(0, RING, cut_first, None)
        spot = lax.broadcasted_iota(jnp.int32, (8, 128), 0) + lax.broadcasted_iota(jnp.int32, (8, 128), 1)
        loss_ref[...] = jnp.where(spot == 0, jnp.broadcast_to(loss, (8, 128)), 0.0)

    outs = [shape_of((RING, rows, width), BF16)] * 8 + [shape_of((8, 128))]
    scratch = [pltpu.VMEM((batch, width), BF16)] + [pltpu.VMEM((width, width), BF16)] * 2
    scratch = scratch + [pltpu.VMEM((batch, width), BF16)] * 3 + [pltpu.VMEM((width, width), BF16)]
    scratch = scratch + [pltpu.SemaphoreType.DMA]
    spaces = [HBM] + [VMEM] * 9
    results = call(kernel, (inputs, labels, *all_a, *all_b), outs, scratch, spaces, limit=32)
    return results[:4], results[4:8], results[8]


def scattered(first, second, after, ordered):
    rows, width = first[0].shape[1:]
    first, second = shifted_copies(first, AXES[0], second, AXES[1])

    def kernel(*refs):
        outs = refs[-8:]
        place = places()

        def block(b, _):
            lines = pl.ds(pl.multiple_of(b * 16, 16), 16)
            for axis, ins, own in ((1, refs[:4], outs[:4]), (0, refs[4:8], outs[4:])):
                for k in range(RING):
                    at = lax.rem(place[axis] + k, RING)
                    total = ins[0][at, lines, :].astype(F32)
                    for i in range(1, RING):
                        total = total + ins[i][at, lines, :].astype(F32)
                    own[k][lines, :] = total.astype(own[k].dtype)

        lax.fori_loop(0, rows // 16, block, None)

    outs = ([shape_of((rows, width))] + [shape_of((rows, width), BF16)] * 3) * 2
    spaces = [VMEM] * 8 + [HBM if ordered else VMEM] * len(after)
    parts = call(kernel, (*first, *second, *after), outs, spaces=spaces)
    return shifted_copies(parts[:4], AXES[1], parts[4:], AXES[0])


def reduce_gradient(parts, moment, tensor, loss, others, members):
    rows, both = moment.shape
    width = both // 2
    scale = width**-0.5
    block = 16

    def kernel(*refs):
        r_refs, refs = refs[:8], refs[8:]
        m_any, p_any, loss_ref = refs[:3]
        other_refs = refs[3 : 3 + len(others)]
        g_any, m_out_any, s_ref, m_ref, p_ref, g_ref, m_out, sems = refs[3 + len(others) :]
        loads = fetch(((m_any, m_ref), (p_any, p_ref)), sems)
        pieces = [
            (slice(b * block, (b + 1) * block), half, slice(q * width // 2, (q + 1) * width // 2))
            for b in range(rows // block)
            for half in range(2)
            for q in range(2)
        ]
        for at, half, own in pieces:
            g = r_refs[4 * half][at, own]
            for i in range(1, RING):
                g = g + r_refs[4 * half + i][at, own].astype(F32)
            g_ref[at, half * width + own.start : half * width + own.stop] = g * scale
        for load in loads:
            load.wait()
        totals = [jnp.zeros((8, 128), F32) for _ in range(8)]
        for at, half, own in pieces:
            lanes = slice(half * width + own.start, half * width + own.stop)
            g = g_ref[at, lanes]
            p = p_ref[at, lanes]
            m = BETA * m_ref[at, lanes] + (1.0 - BETA) * g
            m_out[at, lanes] = m
            for k, product in enumerate((g * g, m * m, p * p, g * m)):
                part = product[:8] + product[8:]
                for j in range(width // 256):
                    totals[4 * half + k] = totals[4 * half + k] + part[:, j * 128 : (j + 1) * 128]
        lines = totals + [loss_ref[...]] + [ref[ref.shape[0] - 8 :, :128] for ref in other_refs]
        spot = lax.broadcasted_iota(jnp.int32, (8, 128), 1)
        tile = jnp.zeros((8, 128), F32)
        for k, line in enumerate(lines):
            column = jnp.sum(line, axis=1, keepdims=True)
            tile = jnp.where(spot == k, column, tile)
        copies = fetch(((g_ref, g_any), (m_out, m_out_any)), sems)
        for i in range(members):
            s_ref[i] = tile
        for copy in copies:
            copy.wait()

    ins = (*parts[0], *parts[1], moment, tensor, loss, *others)
    outs = [pltpu.HBM((rows, both), F32)] * 2 + [shape_of((members, 8, 128))]
    scratch = [pltpu.VMEM((rows, both), F32)] * 4 + [pltpu.SemaphoreType.DMA((2,))]
    spaces = [VMEM] * 8 + [HBM] * 2 + [VMEM] * (1 + len(others))
    return call(kernel, ins, outs, scratch, spaces, [HBM, HBM, VMEM])


def learned_update(sums, theta, hyper_in, hyper_out, gradient, moment, tensor, counts, step, steps, members, classes, last):
    rows, both = gradient.shape
    width = both // 2
    hyp = hyper_in.shape[1]

    def kernel(*refs):
        s_ref, t_ref, in_ref, out_ref = refs[:4]
        g_ref, m_ref, p_ref, sems = scratch_refs
        loads = fetch(((refs[4], g_ref), (refs[5], m_ref), (refs[6], p_ref)), sems)
        total = s_ref[0]
        for i in range(1, members):
            total = total + s_ref[i]
        total = jnp.sum(total, axis=0, keepdims=True)
        means = []
        opening = []
        for k in range(2):
            a, b, c, e = (total[:, 4 * k + j : 4 * k + j + 1] / counts[k] for j in range(4))
            means.append((a, b))
            z = (
                jnp.log(FLOOR + a),
                jnp.log(FLOOR + b),
                jnp.log(1.0 + c),
                e / jnp.sqrt((FLOOR + a) * (FLOOR + b)),
            )
            line = in_ref[4:5, :] * ((step + 1.0) / steps) + in_ref[5:6, :] + in_ref[6 + k : 7 + k, :]
            for j in range(4):
                line = line + z[j] * in_ref[j : j + 1, :]
            opening.append(line)
        opening.append(jnp.zeros((6, hyp), F32))
        opening = jnp.tanh(jnp.concatenate(opening, axis=0))
        columns = opening.T
        share = t_ref.shape[1]
        middle = []
        for k in range(2):
            total_k = jnp.zeros((8, hyp), F32)
            for d in range(members):
                product = columns[d * share : (d + 1) * share, k : k + 1] * t_ref[d]
                for i in range(share // 8):
                    total_k = total_k + product[i * 8 : (i + 1) * 8]
            middle.append(jnp.sum(total_k, axis=0, keepdims=True))
        middle.append(jnp.zeros((6, hyp), F32))
        middle = jnp.tanh(jnp.concatenate(middle, axis=0))
        coeffs = lax.dot_general(
            middle, out_ref[...], BY_COLUMNS, precision=HIGH, preferred_element_type=F32
        )
        for load in loads:
            load.wait()
        column = lax.broadcasted_iota(jnp.int32, (1, width), 1)
        for k in range(2):
            g = [coeffs[k : k + 1, j : j + 1] for j in range(5 * NEURONS + 1)]
            by_g = 1.0 / jnp.sqrt(FLOOR + means[k][0])
            by_m = 1.0 / jnp.sqrt(FLOOR + means[k][1])
            rate = LR_BASE * jnp.exp(g[5 * NEURONS])
            lanes = slice(k * width, (k + 1) * width)
            for b in range(rows // 16):
                at = slice(b * 16, (b + 1) * 16)
                f1 = g_ref[at, lanes]
                f2 = m_ref[at, lanes]
                f3 = p_ref[at, lanes]
                direction = jnp.zeros_like(f3)
                for n in range(NEURONS):
                    inner = (
                        (g[3 * n] * by_g) * f1
                        + (g[3 * n + 1] * by_m) * f2
                        + g[3 * n + 2] * f3
                        + g[3 * NEURONS + n]
                    )
                    direction = direction + g[4 * NEURONS + n] * jnp.maximum(inner, 0.0)
                fresh = f3 - rate * direction
                if last is None:
                    if k == 1:
                        fresh = jnp.where(column < classes, fresh, 0.0)
                    p_ref[at, lanes] = fresh
                    refs[8 + k][at, :] = fresh.astype(BF16)
                elif k == 0:
                    outs[0][0, at, :] = fresh
                    outs[2][0, at, :] = f2
                else:
                    outs[1][0, at, :] = fresh[:, :classes]
                    outs[3][0, at, :] = f2[:, :classes]

    def final_kernel(*refs):
        nonlocal outs, scratch_refs
        scratch_refs = refs[-4:]
        packed_refs, loss_ref = refs[7:-11], refs[-11]
        outs = refs[-10:-4]
        kernel(*refs[:7])
        s_ref = refs[0]
        total = s_ref[0]
        for i in range(1, members):
            total = total + s_ref[i]
        total = jnp.sum(total, axis=0, keepdims=True)
        earlier = jnp.sum(loss_ref[...], axis=(0, 1), keepdims=True)
        own = total[:, 8:9] / batch_total
        tasks = len(packed_refs)
        scores = [(earlier + own) / steps]
        for t in range(1, tasks):
            scores.append(total[:, 8 + t : 9 + t] / batch_total / steps)
        center = scores[0]
        for score in scores[1:]:
            center = center + score
        center = center / tasks
        rows_out = outs[4].shape[0]
        meta = jnp.zeros(outs[4].shape, F32)
        for score, ref in zip(scores, packed_refs):
            meta = meta + (score - center) * ref[:rows_out, :]
        outs[4][...] = meta / (SIGMA * tasks)
        spot = lax.broadcasted_iota(jnp.int32, (1, steps), 1)
        outs[5][...] = jnp.where(spot == 0, earlier, own)

    def first_kernel(*refs):
        nonlocal scratch_refs
        scratch_refs = refs[-4:]
        kernel(*refs[:-4])
        store = fetch(((scratch_refs[2], refs[7]),), scratch_refs[3])
        total = refs[0][0]
        for i in range(1, members):
            total = total + refs[0][i]
        own = jnp.sum(total[:, 8:9], axis=0, keepdims=True) / batch_total
        place = lax.broadcasted_iota(jnp.int32, (8, 128), 0) + lax.broadcasted_iota(jnp.int32, (8, 128), 1)
        refs[10][...] = jnp.where(place == 0, jnp.broadcast_to(own, (8, 128)), 0.0)
        store[0].wait()

    outs = None
    scratch_refs = None
    batch_total = counts[2]
    ins = [sums, theta, hyper_in, hyper_out, gradient, moment, tensor]
    scratch = [pltpu.VMEM((rows, both), F32)] * 3 + [pltpu.SemaphoreType.DMA((3,))]
    spaces = [VMEM] * 4 + [HBM] * 3
    if last is None:
        shapes = [pltpu.HBM((rows, both), F32)] + [shape_of((rows, width), BF16)] * 2 + [shape_of((8, 128))]
        return call(first_kernel, ins, shapes, scratch, spaces, [HBM, VMEM, VMEM, VMEM])
    ins = ins + list(last)
    shapes = [
        shape_of((1, rows, width)),
        shape_of((1, rows, classes)),
        shape_of((1, rows, width)),
        shape_of((1, rows, classes)),
        shape_of((last[0].shape[0] - 8, last[0].shape[1])),
        shape_of((1, steps)),
    ]
    return call(final_kernel, ins, shapes, scratch, spaces + [VMEM] * len(last))


def on_device(
    inputs, labels, w_hidden, w_out, mom_hidden, mom_out, signs, perturb, hyper_in, hyper_mid, hyper_out
):
    members = lax.axis_size(AXES)
    tasks = lax.axis_size("task")
    steps, batch, _ = inputs.shape[1:]
    rows, width = w_hidden.shape[1:]
    classes = w_out.shape[2]
    counts = (float(rows * members * width), float(rows * members * classes), float(batch * members))
    hyper_out = hyper_out.T

    send_a, send_b, signed = prepare(w_hidden, w_out, signs, perturb, hyper_mid)
    local_losses = []
    losses = []
    for step in range(steps):
        all_a, all_b, came = gathered(send_a, send_b)
        if step == 0:
            tensor, moment = side_by_side(w_hidden, w_out, mom_hidden, mom_out, came)
            theta = joined_theta(all_a, all_b, width, hyper_mid.shape[0])
        first, second, loss = forward_backward(inputs, labels, all_a, all_b, step, classes)
        local_losses.append(loss)
        is_last = step == steps - 1
        others = []
        if is_last:
            packed = packed_with(signed, local_losses)
            others = [
                lax.ppermute(packed, "task", [(i, (i + k) % tasks) for i in range(tasks)])
                for k in range(1, tasks)
            ]
        parts = scattered(first, second, others if is_last else [tensor], not is_last)
        gradient, moment, sums = reduce_gradient(parts, moment, tensor, loss, others, members)
        sums = lax.all_to_all(sums, AXES, split_axis=0, concat_axis=0, tiled=True)
        last = (packed, *others, losses[0]) if is_last else None
        results = learned_update(
            sums, theta, hyper_in, hyper_out, gradient, moment, tensor, counts, step, steps, members, classes, last
        )
        if not is_last:
            tensor, send_a, send_b, loss_tile = results
            losses.append(loss_tile)
    new_hidden, new_out, new_mom_hidden, new_mom_out, meta_grad, loss_row = results
    return new_hidden, new_out, new_mom_hidden, new_mom_out, loss_row, meta_grad


def solution(mesh):
    split = Mesh(mesh.devices.reshape(mesh.shape["task"], RING, RING), ("task", *AXES))
    return jax.shard_map(
        on_device,
        mesh=split,
        in_specs=(
            P("task", None, AXES, None),
            P("task", None, AXES),
            P("task", AXES, None),
            P("task", AXES, None),
            P("task", AXES, None),
            P("task", AXES, None),
            P("task"),
            P("task", AXES, None),
            P(),
            P(AXES, None),
            P(),
        ),
        out_specs=(
            P("task", AXES, None),
            P("task", AXES, None),
            P("task", AXES, None),
            P("task", AXES, None),
            P("task", None),
            P(AXES, None),
        ),
        check_vma=False,
    )
```
